32 devices in a mesh: chain: 8 (over z, core), dp: 4 (over y, x).
Axes of the slice: x: 2, y: 2, z: 4, core: 2. Of those that a mesh axis runs over, the one named last changes fastest.
Arguments:
- images_in: float32 [8, 1024, 1024], P('chain', 'dp'), may hold values from -8 to 8
- images_mid: float32 [8, 1024, 1024], P('chain', 'dp'), may hold values from -8 to 8
- images_out: float32 [8, 1024, 1000], P('chain', 'dp'), may hold values from -8 to 8
- ends_in: float32 [2, 1024, 1024], P(None, 'dp'), may hold values from -8 to 8
- ends_mid: float32 [2, 1024, 1024], P(None, 'dp'), may hold values from -8 to 8
- ends_out: float32 [2, 1024, 1000], P(None, 'dp'), may hold values from -8 to 8
- data_pool: bfloat16 [7168, 1024], P('dp'), may hold values from -6 to 6
- batch_rows: int32 [8, 3584], P('chain', 'dp'), may hold values from 0 to 1791
- labels: int32 [8, 3584], P('chain', 'dp'), may hold values from 0 to 999
- climbing: int32 [8], P('chain'), may hold values 0 or 1
Outputs:
- new_in: float32 [8, 1024, 1024], P('chain', 'dp')
- new_mid: float32 [8, 1024, 1024], P('chain', 'dp')
- new_out: float32 [8, 1024, 1000], P('chain', 'dp')
- energies: float32 [8], P('chain')
- arc_share: float32 [8], P('chain')
- bend: float32 [8], P('chain')
The draws below stay inside these ranges and needn't reach their ends.
Inputs may be any that keep to these rules, and one draw needn't show every extreme that they name: batch_rows[i, b] names a row of the pool shard held by dp index b // 896.
All inputs are finite; a program needn't handle non-finite values. No bound on the sum of `climbing` on one device may be relied on, other than what follows from the above.
Results may differ from the reference program's by a relative error of at most 0.0023.
Values may be sent and summed in bfloat16 or wider, within the bound.
A program may use at most 128 MiB of HBM per device.

```python
import jax
import jax.numpy as jnp
from jax import lax

D = 1024
FF = 1024
C = 1000
B_DEV = 896
POOL = 1792
IMAGES = 8
BATCH = 3584
ROWS = 7168


def row_scale(count):
    top = 2.5
    return jnp.exp(jnp.log(top) * jnp.arange(count, dtype=jnp.float32) / (count - 1))


def band_ends(key, tag, shape):
    scale = row_scale(shape[0])[:, None]
    first = jax.random.normal(jax.random.fold_in(key, tag), shape, jnp.float32) * scale
    second = jax.random.normal(jax.random.fold_in(key, tag + 100), shape, jnp.float32) * scale
    return (jnp.clip(first, -7.5, 7.5), jnp.clip(second, -7.5, 7.5))


def band_images(key, tag, shape):
    first, second = band_ends(key, tag, shape)
    scale = row_scale(shape[0])[None, :, None]
    spacing = 1.0 + 2.0 * jnp.arange(IMAGES + 1, dtype=jnp.float32) / IMAGES
    along = jnp.cumsum(spacing)[:IMAGES] / jnp.sum(spacing)
    noise_key = jax.random.fold_in(key, tag + 200)
    noise = 0.03 * jax.random.normal(noise_key, (IMAGES,) + shape, jnp.float32)
    return first[None] + along[:, None, None] * (second - first)[None] + noise * scale


def draw_images_in(key, part):
    return band_images(key, 1, (D, FF))


def draw_images_mid(key, part):
    return band_images(key, 2, (FF, D))


def draw_images_out(key, part):
    return band_images(key, 3, (D, C))


def draw_ends_in(key, part):
    return jnp.stack(band_ends(key, 1, (D, FF)))


def draw_ends_mid(key, part):
    return jnp.stack(band_ends(key, 2, (FF, D)))


def draw_ends_out(key, part):
    return jnp.stack(band_ends(key, 3, (D, C)))


def plant(result, rng, least, high):
    dims = result.shape
    index_at = [jax.random.randint(jax.random.fold_in(rng, axis), (), 0, dims[axis]) for axis in range(len(dims))]
    result = result.at[tuple(index_at)].set(least)
    longest = dims.index(max(dims))
    index_at[longest] = (index_at[longest] + 1) % dims[longest]
    return result.at[tuple(index_at)].set(high)


def steps_of(rng, dims, shards, low, high):
    def one(axis_at, blocks):
        draws = jax.random.uniform(jax.random.fold_in(jax.random.fold_in(rng, 6), axis_at), (blocks,), jnp.float32, low / len(shards), high / len(shards))
        return jnp.repeat(jnp.exp(draws), dims[axis_at] // blocks).reshape((-1,) + (1,) * (len(dims) - axis_at - 1))

    gain = one(*shards[0])
    for cut in shards[1:]:
        gain = gain * one(*cut)
    return gain


def centred(key, dims, width, bound, split=(), kind=jnp.bfloat16):
    factor_of = steps_of(key, dims, split, -0.22, 0.18) if split else 1.0
    values = jax.random.normal(key, dims, jnp.float32) * width * factor_of
    return jnp.minimum(jnp.maximum(values, -bound), bound).astype(kind)


def setup_inputs(seed: int = 0) -> dict:
    seeds = jax.random.split(jax.random.key(seed), 11)
    return {
        "images_in": draw_images_in(jax.random.fold_in(seeds[10], 71), 0),
        "images_mid": draw_images_mid(jax.random.fold_in(seeds[10], 71), 0),
        "images_out": draw_images_out(jax.random.fold_in(seeds[10], 71), 0),
        "ends_in": draw_ends_in(jax.random.fold_in(seeds[10], 71), 0),
        "ends_mid": draw_ends_mid(jax.random.fold_in(seeds[10], 71), 0),
        "ends_out": draw_ends_out(jax.random.fold_in(seeds[10], 71), 0),
        "data_pool": centred(seeds[6], (ROWS, D), 1.0, 6.0, ((0, 4),)),
        "batch_rows": plant(jax.random.randint(seeds[7], (IMAGES, BATCH), 0, POOL), jax.random.fold_in(seeds[7], 1), 0, POOL - 1).astype(jnp.int32),
        "labels": plant(jax.random.randint(seeds[8], (IMAGES, BATCH), 0, C), jax.random.fold_in(seeds[8], 1), 0, C - 1).astype(jnp.int32),
        "climbing": plant((jax.random.randint(seeds[9], (IMAGES,), 0, 4) < 1).astype(jnp.int32), jax.random.fold_in(seeds[9], 1), 0, 1),
    }


SPRING = 0.03
EPS = 1e-06

def silu_slope(pre):
    sig = jax.nn.sigmoid(pre)
    return sig * (1.0 + pre * (1.0 - sig))

def image_terms(packed, data_pool):
    p_in, p_mid, p_out, picks, labs = packed
    w_in = (p_in * D ** (-0.5)).astype(jnp.bfloat16)
    w_mid = (p_mid * FF ** (-0.5)).astype(jnp.bfloat16)
    w_out = (p_out * D ** (-0.5)).astype(jnp.bfloat16)
    owner = (jnp.arange(BATCH, dtype=jnp.int32) // B_DEV).astype(jnp.int32)
    rows = data_pool[owner * POOL + picks]
    pre = jnp.dot(rows, w_in, preferred_element_type=jnp.float32)
    hid = jax.nn.silu(pre).astype(jnp.bfloat16)
    resid = (rows.astype(jnp.float32) + jnp.dot(hid, w_mid, preferred_element_type=jnp.float32)).astype(jnp.bfloat16)
    logits = jnp.dot(resid, w_out, preferred_element_type=jnp.float32)
    target = (labs[:, None] == jnp.arange(C, dtype=jnp.int32)[None, :]).astype(jnp.float32)
    err = logits - target
    norm = 1.0 / (BATCH * C)
    energy = 0.5 * norm * jnp.sum(err * err)
    d_logits = (err * norm).astype(jnp.bfloat16)
    d_resid = jnp.dot(d_logits, w_out.T, preferred_element_type=jnp.float32).astype(jnp.bfloat16)
    d_pre = (jnp.dot(d_resid, w_mid.T, preferred_element_type=jnp.float32) * silu_slope(pre)).astype(jnp.bfloat16)
    g_in = jnp.dot(rows.T, d_pre, preferred_element_type=jnp.float32) * D ** (-0.5)
    g_mid = jnp.dot(hid.T, d_resid, preferred_element_type=jnp.float32) * FF ** (-0.5)
    g_out = jnp.dot(resid.T, d_logits, preferred_element_type=jnp.float32) * D ** (-0.5)
    return (g_in, g_mid, g_out, energy)

def inner(first, second):
    total = jnp.zeros((first[0].shape[0],), jnp.float32)
    for left, right in zip(first, second):
        total = total + lax.optimization_barrier(jnp.sum(left * right, axis=(1, 2)))
    return total

def reference(images_in, images_mid, images_out, ends_in, ends_mid, ends_out, data_pool, batch_rows, labels, climbing):
    g_in, g_mid, g_out, energies = lax.map(lambda packed: image_terms(packed, data_pool), (images_in, images_mid, images_out, batch_rows, labels))
    own = (images_in, images_mid, images_out)
    ends = (ends_in, ends_mid, ends_out)
    grads = (g_in, g_mid, g_out)
    before = tuple((jnp.concatenate([e[0:1], o[:-1]], axis=0) for e, o in zip(ends, own)))
    after = tuple((jnp.concatenate([o[1:], e[1:2]], axis=0) for e, o in zip(ends, own)))
    ahead = tuple((a - o for a, o in zip(after, own)))
    behind = tuple((o - b for o, b in zip(own, before)))
    len_ahead = jnp.sqrt(inner(ahead, ahead) + EPS)
    len_behind = jnp.sqrt(inner(behind, behind) + EPS)
    raw = tuple((a / len_ahead[:, None, None] + b / len_behind[:, None, None] for a, b in zip(ahead, behind)))
    raw_norm = jnp.sqrt(inner(raw, raw) + EPS)
    tau = tuple((r / raw_norm[:, None, None] for r in raw))
    along = inner(grads, tau)
    arc = jnp.cumsum(len_behind)
    band = jnp.sum(len_behind) + len_ahead[-1]
    order = jnp.arange(IMAGES, dtype=jnp.int32)
    target = (order + 1).astype(jnp.float32) / (IMAGES + 1) * band
    coef = jnp.where(climbing == 1, 2.0 * along, along + SPRING * (target - arc) / band)
    force = tuple((-g + coef[:, None, None] * t for g, t in zip(grads, tau)))
    force_len = jnp.sqrt(inner(force, force) + EPS)
    scale = band / (IMAGES + 1) / force_len
    new = tuple((o + scale[:, None, None] * f for o, f in zip(own, force)))
    return (new[0], new[1], new[2], energies, arc / band, 0.5 * raw_norm)
```

```python
import functools

import jax
import jax.numpy as jnp
from jax import lax
from jax.experimental import pallas as pl
from jax.experimental.pallas import tpu as pltpu
from jax.sharding import PartitionSpec as P

SPRING = 0.03
EPS = 1e-06
TILE = 256
LANES = 128
F32 = jnp.float32
BF16 = jnp.bfloat16


def copies_of(count, chain, chunks):
    pairs = count // 2
    gather = (2 + chunks) * (1 + (pairs - 1) + pairs)
    scatter = 3 * chunks * (pairs + (pairs - 1) + 1)
    return gather + scatter + 6 + 2 * (count - 1) + (chain - 1) + 2 + 2


def dot_nn(left, right):
    return jnp.dot(left, right, preferred_element_type=F32)


def dot_nt(left, right):
    return lax.dot_general(left, right, (((1,), (1,)), ((), ())), preferred_element_type=F32)


def dot_tn(left, right):
    return lax.dot_general(left, right, (((0,), (0,)), ((), ())), preferred_element_type=F32)


def fold(value):
    part = jnp.sum(value.reshape(value.shape[0] // 8, 8, value.shape[1]), axis=0)
    total = part[:, :LANES]
    for k in range(1, value.shape[1] // LANES):
        total = total + part[:, k * LANES : (k + 1) * LANES]
    return total


def whole(tile):
    return jnp.sum(tile, axis=(0, 1), keepdims=True)


def kernel(
    n,
    c,
    classes,
    p_in,
    p_mid,
    p_out,
    e_in,
    e_mid,
    e_out,
    pool,
    picks,
    labs,
    climb,
    o_in,
    o_mid,
    o_out,
    o_energy,
    o_arc,
    o_bend,
    own,
    edge,
    thin,
    tau,
    wide,
    stage,
    near,
    before,
    after,
    pool_v,
    hot,
    lab_t,
    lab_out,
    lab_in,
    rows_out,
    rows,
    slope,
    hid,
    resid,
    rows_t,
    hid_t,
    resid_t,
    dlog,
    dres,
    grad,
    from_core,
    from_pair,
    last,
    power,
    sums,
    spans,
    late,
    load_sem,
    send_sem,
    recv_sem,
):
    ci, me = lax.axis_index("chain"), lax.axis_index("dp")
    pairs = n // 2
    core, side = lax.rem(ci, 2), lax.rem(me, 2)
    pair = me // 2
    leads = core == side
    moves = core != side
    cross = (ci + 1 - 2 * core, me + 1 - 2 * side)
    twin = (ci + 1 - 2 * core, me)
    block, width = own.shape[1], own.shape[2]
    depth = n * block
    step = min(32, block)
    batch = rows.shape[0]
    tiles = width // TILE
    factor = (depth**-0.5, width**-0.5, depth**-0.5)
    norm = 1.0 / (batch * n * classes)
    counter = [0]

    def remote(src, dst, to):
        k = counter[0]
        counter[0] += 1
        copy = pltpu.make_async_remote_copy(
            src_ref=src,
            dst_ref=dst,
            send_sem=send_sem.at[k],
            recv_sem=recv_sem.at[k],
            device_id=to,
            device_id_type=pl.DeviceIdType.MESH,
        )
        return copy

    def pair_at(d):
        return lax.rem(pair + d, pairs)

    barrier = pltpu.get_barrier_semaphore()
    for d in range(1, n):
        pl.semaphore_signal(
            barrier, inc=1, device_id=(ci, lax.rem(me + d, n)), device_id_type=pl.DeviceIdType.MESH
        )
    for d in range(1, c):
        pl.semaphore_signal(
            barrier, inc=1, device_id=(lax.rem(ci + d, c), me), device_id_type=pl.DeviceIdType.MESH
        )

    pl.semaphore_signal(barrier, inc=1, device_id=cross, device_id_type=pl.DeviceIdType.MESH)

    end = jnp.where(ci == 0, 0, 1)
    loads = [
        pltpu.make_async_copy(p_in.at[0], own.at[0], load_sem.at[0]),
        pltpu.make_async_copy(p_mid.at[0], own.at[1], load_sem.at[1]),
        pltpu.make_async_copy(p_out.at[0], thin.at[0, pl.ds(0, classes)], load_sem.at[2]),
        pltpu.make_async_copy(pool, pool_v, load_sem.at[3]),
        pltpu.make_async_copy(e_in.at[end], edge.at[0], load_sem.at[4]),
        pltpu.make_async_copy(e_mid.at[end], edge.at[1], load_sem.at[5]),
        pltpu.make_async_copy(e_out.at[end], thin.at[1, pl.ds(0, classes)], load_sem.at[6]),
    ]
    for load in loads:
        load.start()

    def turned(into, thin_at):
        @pl.loop(0, width // LANES)
        def _(k):
            at = pl.ds(pl.multiple_of(k * LANES, LANES), LANES)
            into[:, at] = thin[thin_at, at, :].T

    def blanked(thin_at):
        if classes < width:
            thin[thin_at, pl.ds(classes, width - classes), :] = jnp.zeros(
                (width - classes, block), F32
            )

    def lowered(m):
        def body(r, _):
            off = pl.multiple_of(r * step, step)
            value = own[m, pl.ds(off, step), :]
            low = (value * factor[m]).astype(BF16)
            stage[m, pl.ds(off, step), :] = low

            @pl.when(leads)
            def _():
                wide[m, pl.ds(pl.multiple_of(me * block + off, step), step), :] = low

            near[m, pl.ds(off, step), :] = value.astype(BF16)
            return 0

        lax.fori_loop(0, block // step, body, 0)

    def column(t):
        return pl.ds(pl.multiple_of(t * TILE, TILE), TILE)

    everything = pl.ds(0, width)
    tail = TILE if batch > TILE else 0
    blocks = [pl.ds(0, batch - tail)] + ([pl.ds(batch - tail, tail)] if tail else [])

    def piece(ref, m, index, at=everything):
        return ref.at[m, pl.ds(pl.multiple_of(index * block, block), block), at]

    started = []

    def begin(copy):
        copy.start()
        started.append(copy)
        return copy

    hop, across, over = {}, {}, {}
    swapped = []

    def swap(src, dst):
        copy = remote(src, dst, cross)
        swapped.append(copy)
        return copy

    def send(*copies):
        @pl.when(moves)
        def _():
            for copy in copies:
                copy.start()

    def arrive(*copies):
        @pl.when(moves)
        def _():
            for copy in copies:
                copy.wait_recv()

    def prepare(key, m, at=everything):
        hop[key] = swap(stage.at[m, :, at], piece(wide, m, me, at))
        held = piece(wide, m, 2 * pair + core, at)
        across[key] = [
            remote(held, held, (ci, 2 * pair_at(d) + side)) for d in range(1, pairs)
        ]
        over[key] = [remote(held, held, twin)]
        started.extend(across[key] + over[key])

    def spread(key):
        for copy in across[key] + over[key][:1]:
            copy.start()

    def spread_own(*keys):
        @pl.when(leads)
        def _():
            for key in keys:
                spread(key)

    def spread_moved(*keys):
        @pl.when(moves)
        def _():
            for key in keys:
                hop[key].wait_recv()
                spread(key)

    def forward(key, m, at=everything):
        for d in range(1, pairs):
            across[key][d - 1].wait_recv()
            held = piece(wide, m, 2 * pair_at(pairs - d) + core, at)
            over[key].append(begin(remote(held, held, twin)))

    def gathered(key):
        for copy in over[key]:
            copy.wait_recv()

    def cols(t):
        return pl.ds(t * TILE, TILE)

    parts = [(2, t) for t in range(tiles)]
    for m in range(2):
        prepare(m, m)
    for key in parts:
        prepare(key, 2, cols(key[1]))

    loads[0].wait()
    lowered(0)
    pl.semaphore_wait(barrier, n - 1 + c - 1 + 1)
    send(hop[0])
    spread_own(0)
    loads[1].wait()
    lowered(1)
    send(hop[1])
    spread_own(1)
    blanked(0)
    blanked(1)
    loads[2].wait()
    turned(own.at[2], 0)
    lowered(2)
    spread_own(*parts)

    ups = [remote(near.at[m], before.at[m], (lax.rem(ci + 1, c), me)) for m in range(3)]
    downs = [remote(near.at[m], after.at[m], (lax.rem(ci + c - 1, c), me)) for m in range(3)]
    has_next, has_prev = ci < c - 1, ci > 0

    @pl.when(has_next)
    def _():
        for copy in ups:
            copy.start()

    @pl.when(has_prev)
    def _():
        for copy in downs:
            copy.start()

    lab_rows = jnp.broadcast_to(labs[...], (8, batch))
    lab_out[...] = lab_rows

    @pl.when(leads)
    def _():
        lab_in[...] = lab_rows

    lab_swap = swap(lab_out, lab_in)
    send(lab_swap)
    row_of = jnp.broadcast_to(picks[...], (LANES, batch)).T
    lane = lax.broadcasted_iota(jnp.int32, (batch, LANES), 1)
    for k in range(pool_v.shape[0] // LANES):
        hot[:, k * LANES : (k + 1) * LANES] = (row_of == lane + k * LANES).astype(F32).astype(BF16)
    loads[3].wait()
    row_swap = []
    for b, rs in enumerate(blocks):

        @pl.loop(0, tiles)
        def _(t):
            at = column(t)
            picked = dot_nn(hot[rs, :], pool_v[:, at]).astype(BF16)
            rows_out[rs, at] = picked

            @pl.when(leads)
            def _():
                rows[rs, at] = picked

        row_swap.append(swap(rows_out.at[rs], rows.at[rs]))
        send(row_swap[b])
        if b == 0:
            send(hop[parts[0]])
    send(*[hop[key] for key in parts[1:]])

    spread_moved(0, 1)
    forward(0, 0)
    for load in loads[4:]:
        load.wait()
    turned(edge.at[2], 1)

    @pl.when(has_prev)
    def _():
        for copy in ups:
            copy.wait_recv()

    @pl.when(has_next)
    def _():
        for copy in downs:
            copy.wait_recv()

    def differences(m, at):
        mine = own[m, at, :]
        fixed = edge[m, at, :]
        left = jnp.where(ci == 0, fixed, before[m, at, :].astype(F32))
        right = jnp.where(ci == c - 1, fixed, after[m, at, :].astype(F32))
        return right - mine, mine - left

    zero = jnp.zeros((8, LANES), F32)

    def span_sums(m, carry):
        def body(r, carry):
            ahead, behind = differences(m, pl.ds(pl.multiple_of(r * step, step), step))
            return (
                carry[0] + fold(ahead * ahead),
                carry[1] + fold(behind * behind),
                carry[2] + fold(ahead * behind),
            )

        return lax.fori_loop(0, block // step, body, carry)

    carry = (zero, zero, zero)
    for m in range(3):
        carry = span_sums(m, carry)
    for k in range(3):
        sums[me, k] = carry[k]
    sums_out = [
        begin(remote(sums.at[me], sums.at[me], (ci, lax.rem(me + d, n)))) for d in range(1, n)
    ]

    gathered(0)
    arrive(lab_swap)
    lab_t[...] = jnp.broadcast_to(lab_in[...][0:1, :], (LANES, batch)).T

    def activate(rs):
        @pl.loop(0, tiles)
        def _(t):
            at = column(t)
            pre = dot_nn(rows[rs, :], wide[0, :, at])
            sig = jax.nn.sigmoid(pre)
            value = (pre * sig).astype(BF16)
            hid[rs, at] = value
            hid_t[at, rs] = value.T
            slope[rs, at] = sig * (1.0 + pre * (1.0 - sig))

    def residual(rs):
        @pl.loop(0, tiles)
        def _(t):
            at = column(t)
            value = (rows[rs, at].astype(F32) + dot_nn(hid[rs, :], wide[1, :, at])).astype(BF16)
            resid[rs, at] = value
            resid_t[at, rs] = value.T

    for b, rs in enumerate(blocks):
        arrive(row_swap[b])
        activate(rs)
        if b == 0:
            spread_moved(parts[0])
            forward(1, 1)
            gathered(1)
        residual(rs)

    if tiles > 1:
        spread_moved(parts[1])
    forward(parts[0], 2, cols(0))

    def classify(t, energy):
        at = column(t)
        logits = dot_nn(resid[...], wide[2, :, at])
        out = []
        for k in range(TILE // LANES):
            target = (lab_t[...] == lane + (t * TILE + k * LANES)).astype(F32)
            err = logits[:, k * LANES : (k + 1) * LANES] - target
            energy = energy + fold(err * err)
            out.append((err * norm).astype(BF16))
        dlog[:, at] = jnp.concatenate(out, axis=1)
        return energy

    def product(m, left_t, right, at):
        half = depth // 2

        @pl.loop(0, 2)
        def _(r):
            of = pl.ds(pl.multiple_of(r * half, half), half)
            grad[m, of, at] = dot_nn(left_t[of, :], right[:, at]).astype(BF16)

    to_core, to_pair, to_home = {}, {}, {}

    def scatter(key, m, at):
        to_core[key] = [
            begin(remote(piece(grad, m, 2 * q + 1 - core, at), from_core.at[m, q, :, at], twin))
            for q in range(pairs)
        ]
        to_pair[key] = []
        for d in range(1, pairs):
            q = pair_at(d)
            held = piece(grad, m, 2 * q + core, at)
            to_pair[key].append(remote(held, from_pair.at[m, d - 1, :, at], (ci, 2 * q + side)))
        started.extend(to_pair[key])
        held = piece(grad, m, 2 * pair + core, at)
        to_home[key] = swap(held, last.at[m, :, at])

    def combine(m, into, index, terms, at):
        @pl.loop(0, block // step)
        def _(r):
            off = pl.multiple_of(r * step, step)
            of = pl.ds(pl.multiple_of(index * block + off, step), step)
            total = grad[m, of, at].astype(F32)
            for term in terms:
                total = total + term[pl.ds(off, step), :].astype(F32)
            into[pl.ds(off, step), :] = total.astype(BF16)

    def scatter_on(key, m, at):
        for copy in to_core[key]:
            copy.wait_recv()
        for d in range(1, pairs):
            q = pair_at(d)
            held = piece(grad, m, 2 * q + core, at)
            combine(m, held, 2 * q + core, [from_core.at[m, q, :, at]], at)
            to_pair[key][d - 1].start()

    def scatter_home(key, m, at):
        for copy in to_pair[key]:
            copy.wait_recv()
        terms = [from_core.at[m, pair, :, at]]
        terms += [from_pair.at[m, d, :, at] for d in range(pairs - 1)]

        @pl.when(leads)
        def _():
            combine(m, last.at[m, :, at], 2 * pair + core, terms, at)

        @pl.when(moves)
        def _():
            combine(m, piece(grad, m, 2 * pair + core, at), 2 * pair + core, terms, at)
            to_home[key].start()

    def moved_on(key, m, at):
        @pl.when(moves)
        def _():
            scatter_on(key, m, at)

    def led_on(key, m, at):
        @pl.when(leads)
        def _():
            scatter_on(key, m, at)

    energy = zero
    for t in range(tiles):
        gathered(parts[t])
        energy = classify(t, energy)
        if t + 2 < tiles:
            spread_moved(parts[t + 2])
        product(2, resid_t, dlog, cols(t))
        scatter((2, t), 2, cols(t))
        if t + 1 < tiles:
            forward(parts[t + 1], 2, cols(t + 1))
        if t > 0:
            moved_on((2, t - 1), 2, cols(t - 1))
    moved_on((2, tiles - 1), 2, cols(tiles - 1))

    power[0] = energy * (0.5 * norm)
    power_swap = swap(power.at[0], power.at[1])
    send(power_swap)

    for t in range(tiles):
        at = cols(t)
        dres[:, at] = dot_nt(dlog[...], wide[2, at, :]).astype(BF16)
        led_on((2, t), 2, at)
        product(1, hid_t, dres, at)
        scatter((1, t), 1, at)
        if t > 0:
            scatter_on((1, t - 1), 1, cols(t - 1))

    @pl.loop(0, tiles)
    def _(t):
        at = column(t)
        rows_t[at, :] = rows[:, at].T

    scatter_on((1, tiles - 1), 1, cols(tiles - 1))

    for t in range(tiles):
        at = cols(t)
        dlog[:, at] = (dot_nt(dres[...], wide[1, at, :]) * slope[:, at]).astype(BF16)
        product(0, rows_t, dlog, at)
        scatter((0, t), 0, at)
        if t > 0:
            scatter_on((0, t - 1), 0, cols(t - 1))
    scatter_on((0, tiles - 1), 0, cols(tiles - 1))

    for copy in sums_out:
        copy.wait_recv()

    def over_dp(ref, k):
        total = ref[0, k]
        for j in range(1, n):
            total = total + ref[j, k]
        return whole(total)

    sq_ahead, sq_behind, mixed = (over_dp(sums, k) for k in range(3))
    len_ahead = jnp.sqrt(sq_ahead + EPS)
    len_behind = jnp.sqrt(sq_behind + EPS)
    raw_sq = (
        sq_ahead / (len_ahead * len_ahead)
        + sq_behind / (len_behind * len_behind)
        + 2.0 * mixed / (len_ahead * len_behind)
    )
    raw_len = jnp.sqrt(raw_sq + EPS)
    spans[ci, 0] = jnp.broadcast_to(len_behind, (8, LANES))
    spans[ci, 1] = jnp.broadcast_to(len_ahead, (8, LANES))
    spans_out = [
        begin(remote(spans.at[ci], spans.at[ci], (lax.rem(ci + d, c), me))) for d in range(1, c)
    ]
    by_ahead = 1.0 / (len_ahead * raw_len)
    by_behind = 1.0 / (len_behind * raw_len)

    for m in range(3):

        def body(r, _, m=m):
            at = pl.ds(pl.multiple_of(r * step, step), step)
            ahead, behind = differences(m, at)
            tau[m, at, :] = ahead * by_ahead + behind * by_behind
            return 0

        lax.fori_loop(0, block // step, body, 0)

    for copy in spans_out:
        copy.wait_recv()
    arc = jnp.zeros((1, 1), F32)
    band = jnp.zeros((1, 1), F32)
    for k in range(c):
        length = spans[k, 0, 0:1, 0:1]
        arc = arc + jnp.where(k <= ci, length, 0.0)
        band = band + length
    band = band + spans[c - 1, 1, 0:1, 0:1]
    arrive(power_swap)

    def finish(key, m, cs, carry):
        arrive(to_home[key])

        def body(r, carry):
            at = pl.ds(pl.multiple_of(r * step, step), step)
            total = last[m, at, cs].astype(F32) * factor[m]
            edge[m, at, cs] = total
            return carry[0] + fold(total * tau[m, at, cs]), carry[1] + fold(total * total)

        return lax.fori_loop(0, block // step, body, carry)

    carry = (zero, zero)
    queue = [(m, t) for m in (2, 1, 0) for t in range(tiles)]
    lag = 2
    for i in range(len(queue) + lag):
        if i < len(queue):
            m, t = queue[i]
            scatter_home((m, t), m, cols(t))
        if i >= lag:
            m, t = queue[i - lag]
            carry = finish((m, t), m, cols(t), carry)
    late[me, 0] = carry[0]
    late[me, 1] = carry[1]
    late[me, 2] = jnp.where(leads, power[0], power[1])
    late_out = [
        begin(remote(late.at[me], late.at[me], (ci, lax.rem(me + d, n)))) for d in range(1, n)
    ]
    for copy in late_out:
        copy.wait_recv()
    along, g_g, energy_all = (over_dp(late, k) for k in range(3))

    goal = (ci + 1).astype(F32) / (c + 1) * band
    coef = jnp.where(jnp.full((1, 1), climb[0]) == 1, 2.0 * along, along + SPRING * (goal - arc) / band)
    tau_sq = raw_sq / (raw_sq + EPS)
    force_sq = g_g - 2.0 * coef * along + coef * coef * tau_sq
    scale = band / (c + 1) / jnp.sqrt(force_sq + EPS)
    push = scale * coef
    o_energy[0] = energy_all[0, 0]
    o_arc[0] = (arc / band)[0, 0]
    o_bend[0] = (0.5 * raw_len)[0, 0]

    stores = []
    for m, out in ((2, o_out), (1, o_mid), (0, o_in)):
        if m == 2:

            @pl.loop(0, width // LANES)
            def _(k):
                at = pl.ds(pl.multiple_of(k * LANES, LANES), LANES)
                new = own[2, :, at] + (push * tau[2, :, at] - scale * edge[2, :, at])
                thin[0, at, :] = new.T

            source = thin.at[0, pl.ds(0, classes)]
        else:

            @pl.loop(0, block // step)
            def _(r):
                at = pl.ds(pl.multiple_of(r * step, step), step)
                tau[m, at, :] = own[m, at, :] + (push * tau[m, at, :] - scale * edge[m, at, :])

            source = tau.at[m]
        copy = pltpu.make_async_copy(source, out.at[0], load_sem.at[m])
        copy.start()
        stores.append(copy)

    @pl.when(has_next)
    def _():
        for copy in ups:
            copy.wait_send()

    @pl.when(has_prev)
    def _():
        for copy in downs:
            copy.wait_send()

    @pl.when(moves)
    def _():
        for copy in swapped:
            copy.wait_send()

    for copy in started:
        copy.wait_send()
    for copy in stores:
        copy.wait()


def on_device(
    n,
    c,
    images_in,
    images_mid,
    images_out,
    ends_in,
    ends_mid,
    ends_out,
    data_pool,
    batch_rows,
    labels,
    climbing,
):
    block, width = images_in.shape[1], images_in.shape[2]
    classes = images_out.shape[2]
    depth = n * block
    batch = batch_rows.shape[1]
    pairs = n // 2
    copies = copies_of(n, c, width // TILE)
    vmem = pl.BlockSpec(memory_space=pltpu.VMEM)
    anywhere = pl.BlockSpec(memory_space=pl.ANY)
    scalar = pl.BlockSpec(memory_space=pltpu.SMEM)
    small = jax.ShapeDtypeStruct((1,), F32)
    outs = pl.pallas_call(
        functools.partial(kernel, n, c, classes),
        out_shape=(
            jax.ShapeDtypeStruct(images_in.shape, F32),
            jax.ShapeDtypeStruct(images_mid.shape, F32),
            jax.ShapeDtypeStruct((1, classes, block), F32),
            small,
            small,
            small,
        ),
        in_specs=[anywhere] * 7 + [vmem] * 2 + [scalar],
        out_specs=[anywhere] * 3 + [scalar] * 3,
        scratch_shapes=[
            pltpu.VMEM((3, block, width), F32),
            pltpu.VMEM((3, block, width), F32),
            pltpu.VMEM((2, width, block), F32),
            pltpu.VMEM((3, block, width), F32),
            pltpu.VMEM((3, depth, width), BF16),
            pltpu.VMEM((3, block, width), BF16),
            pltpu.VMEM((3, block, width), BF16),
            pltpu.VMEM((3, block, width), BF16),
            pltpu.VMEM((3, block, width), BF16),
            pltpu.VMEM(data_pool.shape, BF16),
            pltpu.VMEM((batch, data_pool.shape[0]), BF16),
            pltpu.VMEM((batch, LANES), jnp.int32),
            pltpu.VMEM((8, batch), jnp.int32),
            pltpu.VMEM((8, batch), jnp.int32),
            pltpu.VMEM((batch, depth), BF16),
            pltpu.VMEM((batch, depth), BF16),
            pltpu.VMEM((batch, width), F32),
            pltpu.VMEM((batch, width), BF16),
            pltpu.VMEM((batch, depth), BF16),
            pltpu.VMEM((depth, batch), BF16),
            pltpu.VMEM((width, batch), BF16),
            pltpu.VMEM((depth, batch), BF16),
            pltpu.VMEM((batch, width), BF16),
            pltpu.VMEM((batch, depth), BF16),
            pltpu.VMEM((3, depth, width), BF16),
            pltpu.VMEM((3, pairs, block, width), BF16),
            pltpu.VMEM((3, max(pairs - 1, 1), block, width), BF16),
            pltpu.VMEM((3, block, width), BF16),
            pltpu.VMEM((2, 8, LANES), F32),
            pltpu.VMEM((n, 3, 8, LANES), F32),
            pltpu.VMEM((c, 2, 8, LANES), F32),
            pltpu.VMEM((n, 3, 8, LANES), F32),
            pltpu.SemaphoreType.DMA((7,)),
            pltpu.SemaphoreType.DMA((copies,)),
            pltpu.SemaphoreType.DMA((copies,)),
        ],
        compiler_params=pltpu.CompilerParams(
            collective_id=0, has_side_effects=True, vmem_limit_bytes=63 * 1024 * 1024
        ),
    )(
        images_in,
        images_mid,
        jnp.swapaxes(images_out, 1, 2),
        ends_in,
        ends_mid,
        jnp.swapaxes(ends_out, 1, 2),
        data_pool,
        batch_rows,
        labels,
        climbing,
    )
    return (outs[0], outs[1], jnp.swapaxes(outs[2], 1, 2), *outs[3:])


def solution(mesh):
    placed = (
        P("chain", "dp", None),
        P("chain", "dp", None),
        P("chain", "dp", None),
        P(None, "dp", None),
        P(None, "dp", None),
        P(None, "dp", None),
        P("dp", None),
        P("chain", "dp"),
        P("chain", "dp"),
        P("chain"),
    )
    return jax.shard_map(
        functools.partial(on_device, mesh.shape["dp"], mesh.shape["chain"]),
        mesh=mesh,
        in_specs=placed,
        out_specs=(
            P("chain", "dp", None),
            P("chain", "dp", None),
            P("chain", "dp", None),
            P("chain"),
            P("chain"),
            P("chain"),
        ),
        check_vma=False,
    )
```

```python
import functools

import jax
import jax.numpy as jnp
from jax import lax
from jax.experimental import pallas as pl
from jax.experimental.pallas import tpu as pltpu
from jax.sharding import PartitionSpec as P

SPRING = 0.03
EPS = 1e-06
TILE = 256
LANES = 128
F32 = jnp.float32
BF16 = jnp.bfloat16


def copies_of(count, chain, chunks, rows):
    pairs = count // 2
    gather = 3 * (1 + (pairs - 1) + pairs)
    scatter = 3 * chunks * (pairs + (pairs - 1) + 1)
    return gather + scatter + 6 + 2 * (count - 1) + (chain - 1) + 2 + rows


def dot_nn(left, right):
    return jnp.dot(left, right, preferred_element_type=F32)


def dot_nt(left, right):
    return lax.dot_general(left, right, (((1,), (1,)), ((), ())), preferred_element_type=F32)


def dot_tn(left, right):
    return lax.dot_general(left, right, (((0,), (0,)), ((), ())), preferred_element_type=F32)


def fold(value):
    part = jnp.sum(value.reshape(value.shape[0] // 8, 8, value.shape[1]), axis=0)
    total = part[:, :LANES]
    for k in range(1, value.shape[1] // LANES):
        total = total + part[:, k * LANES : (k + 1) * LANES]
    return total


def whole(tile):
    return jnp.sum(tile, axis=(0, 1), keepdims=True)


def kernel(
    n,
    c,
    classes,
    p_in,
    p_mid,
    p_out,
    e_in,
    e_mid,
    e_out,
    pool,
    picks,
    labs,
    climb,
    o_in,
    o_mid,
    o_out,
    o_small,
    own,
    edge,
    thin,
    tau_out,
    wide,
    stage,
    near,
    before,
    after,
    pool_v,
    lab_t,
    lab_out,
    lab_in,
    rows_out,
    rows,
    slope,
    hid,
    resid,
    rows_t,
    hid_t,
    resid_t,
    dlog,
    dres,
    grad,
    from_core,
    from_pair,
    last,
    power,
    sums,
    spans,
    late,
    load_sem,
    send_sem,
    recv_sem,
):
    ci, me = lax.axis_index("chain"), lax.axis_index("dp")
    pairs = n // 2
    core, side = lax.rem(ci, 2), lax.rem(me, 2)
    pair = me // 2
    leads = core == side
    moves = core != side
    cross = (ci + 1 - 2 * core, me + 1 - 2 * side)
    twin = (ci + 1 - 2 * core, me)
    block, width = own.shape[1], own.shape[2]
    depth = n * block
    step = min(32, block)
    batch = rows.shape[0]
    tiles = width // TILE
    factor = (depth**-0.5, width**-0.5, depth**-0.5)
    norm = 1.0 / (batch * n * classes)
    counter = [0]
    tau = [o_in.at[0], o_mid.at[0], tau_out]

    def remote(src, dst, to):
        k = counter[0]
        counter[0] += 1
        copy = pltpu.make_async_remote_copy(
            src_ref=src,
            dst_ref=dst,
            send_sem=send_sem.at[k],
            recv_sem=recv_sem.at[k],
            device_id=to,
            device_id_type=pl.DeviceIdType.MESH,
        )
        return copy

    def pair_at(d):
        return lax.rem(pair + d, pairs)
    barrier = pltpu.get_barrier_semaphore()
    for d in range(1, n):
        pl.semaphore_signal(
            barrier, inc=1, device_id=(ci, lax.rem(me + d, n)), device_id_type=pl.DeviceIdType.MESH
        )
    for d in range(1, c):
        pl.semaphore_signal(
            barrier, inc=1, device_id=(lax.rem(ci + d, c), me), device_id_type=pl.DeviceIdType.MESH
        )

    pl.semaphore_signal(barrier, inc=1, device_id=cross, device_id_type=pl.DeviceIdType.MESH)

    end = jnp.where(ci == 0, 0, 1)
    loads = [
        pltpu.make_async_copy(p_in.at[0], own.at[0], load_sem.at[0]),
        pltpu.make_async_copy(p_mid.at[0], own.at[1], load_sem.at[1]),
        pltpu.make_async_copy(p_out.at[0], thin.at[0, pl.ds(0, classes)], load_sem.at[2]),
        pltpu.make_async_copy(pool, pool_v, load_sem.at[3]),
        pltpu.make_async_copy(e_in.at[end], edge.at[0], load_sem.at[4]),
        pltpu.make_async_copy(e_mid.at[end], edge.at[1], load_sem.at[5]),
        pltpu.make_async_copy(e_out.at[end], thin.at[1, pl.ds(0, classes)], load_sem.at[6]),
    ]
    for load in loads:
        load.start()

    def turned(into, thin_at):
        @pl.loop(0, width // LANES)
        def _(k):
            at = pl.ds(pl.multiple_of(k * LANES, LANES), LANES)
            into[:, at] = thin[thin_at, at, :].T

    def blanked(thin_at):
        if classes < width:
            thin[thin_at, pl.ds(classes, width - classes), :] = jnp.zeros(
                (width - classes, block), F32
            )

    def lowered(m):
        def body(r, _):
            off = pl.multiple_of(r * step, step)
            value = own[m, pl.ds(off, step), :]
            low = (value * factor[m]).astype(BF16)
            stage[m, pl.ds(off, step), :] = low

            @pl.when(leads)
            def _():
                wide[m, pl.ds(pl.multiple_of(me * block + off, step), step), :] = low

            near[m, pl.ds(off, step), :] = value.astype(BF16)
            return 0

        lax.fori_loop(0, block // step, body, 0)

    def column(t):
        return pl.ds(pl.multiple_of(t * TILE, TILE), TILE)

    everything = pl.ds(0, width)
    cuts = [0] + [at for at in (batch - 2 * TILE, batch - TILE) if at > 0] + [batch]
    blocks = [pl.ds(low, high - low) for low, high in zip(cuts[:-1], cuts[1:])]

    def piece(ref, m, index, at=everything):
        return ref.at[m, pl.ds(pl.multiple_of(index * block, block), block), at]

    started = []

    def begin(copy):
        copy.start()
        started.append(copy)
        return copy

    hop, across, over = {}, {}, {}
    swapped = []

    def swap(src, dst):
        copy = remote(src, dst, cross)
        swapped.append(copy)
        return copy

    def send(*copies):
        @pl.when(moves)
        def _():
            for copy in copies:
                copy.start()

    def arrive(*copies):
        @pl.when(moves)
        def _():
            for copy in copies:
                copy.wait_recv()

    def prepare(key, m, at=everything):
        hop[key] = swap(stage.at[m, :, at], piece(wide, m, me, at))
        held = piece(wide, m, 2 * pair + core, at)
        across[key] = [
            remote(held, held, (ci, 2 * pair_at(d) + side)) for d in range(1, pairs)
        ]
        over[key] = [remote(held, held, twin)]
        started.extend(across[key] + over[key])

    def spread(key):
        for copy in across[key] + over[key][:1]:
            copy.start()

    def spread_own(*keys):
        @pl.when(leads)
        def _():
            for key in keys:
                spread(key)

    def spread_moved(*keys):
        @pl.when(moves)
        def _():
            for key in keys:
                hop[key].wait_recv()
                spread(key)

    def forward(key, m, at=everything):
        for d in range(1, pairs):
            across[key][d - 1].wait_recv()
            held = piece(wide, m, 2 * pair_at(pairs - d) + core, at)
            over[key].append(begin(remote(held, held, twin)))

    def gathered(key):
        for copy in over[key]:
            copy.wait_recv()

    def cols(t):
        return pl.ds(t * TILE, TILE)

    for m in range(3):
        prepare(m, m)
    loads[0].wait()
    lowered(0)
    pl.semaphore_wait(barrier, n - 1 + c - 1 + 1)
    send(hop[0])
    spread_own(0)
    loads[1].wait()
    lowered(1)
    send(hop[1])
    spread_own(1)
    blanked(0)
    blanked(1)
    loads[2].wait()
    turned(own.at[2], 0)
    lowered(2)
    send(hop[2])
    spread_own(2)

    ups = [remote(near.at[m], before.at[m], (lax.rem(ci + 1, c), me)) for m in range(3)]
    downs = [remote(near.at[m], after.at[m], (lax.rem(ci + c - 1, c), me)) for m in range(3)]
    has_next, has_prev = ci < c - 1, ci > 0

    @pl.when(has_next)
    def _():
        for copy in ups:
            copy.start()

    @pl.when(has_prev)
    def _():
        for copy in downs:
            copy.start()
    lab_rows = jnp.broadcast_to(labs[...], (8, batch))
    lab_out[...] = lab_rows

    @pl.when(leads)
    def _():
        lab_in[...] = lab_rows

    lab_swap = swap(lab_out, lab_in)
    send(lab_swap)
    row_of = jnp.broadcast_to(picks[...], (LANES, batch)).T
    lane = lax.broadcasted_iota(jnp.int32, (batch, LANES), 1)
    supply = pool_v.shape[0]
    for k in range(supply // LANES):
        m, at = k * LANES // width, k * LANES % width
        grad[m, 0:batch, at : at + LANES] = (row_of == lane + k * LANES).astype(F32).astype(BF16)
    reach = [(m, min(width, supply - m * width)) for m in range(-(-supply // width))]

    def picked_of(rs, at):
        return sum(
            dot_nn(grad[m, rs, 0:size], pool_v[pl.ds(m * width, size), at]) for m, size in reach
        )

    loads[3].wait()
    row_swap = []
    for b, rs in enumerate(blocks):

        @pl.loop(0, tiles)
        def _(t):
            at = column(t)
            picked = picked_of(rs, at).astype(BF16)
            rows_out[rs, at] = picked

            @pl.when(leads)
            def _():
                rows[rs, at] = picked

        row_swap.append(swap(rows_out.at[rs], rows.at[rs]))
        send(row_swap[b])
    spread_moved(0, 1, 2)
    forward(0, 0)
    for load in loads[4:]:
        load.wait()
    turned(edge.at[2], 1)

    @pl.when(has_prev)
    def _():
        for copy in ups:
            copy.wait_recv()

    @pl.when(has_next)
    def _():
        for copy in downs:
            copy.wait_recv()

    def differences(m, at):
        mine = own[m, at, :]
        fixed = edge[m, at, :]
        left = jnp.where(ci == 0, fixed, before[m, at, :].astype(F32))
        right = jnp.where(ci == c - 1, fixed, after[m, at, :].astype(F32))
        return right - mine, mine - left
    zero = jnp.zeros((8, LANES), F32)

    def span_sums(m, carry):
        def body(r, carry):
            ahead, behind = differences(m, pl.ds(pl.multiple_of(r * step, step), step))
            return (
                carry[0] + fold(ahead * ahead),
                carry[1] + fold(behind * behind),
                carry[2] + fold(ahead * behind),
            )

        return lax.fori_loop(0, block // step, body, carry)

    carry = (zero, zero, zero)
    for m in range(3):
        carry = span_sums(m, carry)
    for k in range(3):
        sums[me, k] = carry[k]
    sums_out = [
        begin(remote(sums.at[me], sums.at[me], (ci, lax.rem(me + d, n)))) for d in range(1, n)
    ]
    gathered(0)
    arrive(lab_swap)
    lab_t[...] = jnp.broadcast_to(lab_in[...][0:1, :], (LANES, batch)).T

    def activate(rs):
        @pl.loop(0, tiles)
        def _(t):
            at = column(t)
            pre = dot_nn(rows[rs, :], wide[0, :, at])
            sig = jax.nn.sigmoid(pre)
            value = (pre * sig).astype(BF16)
            hid[rs, at] = value
            hid_t[at, rs] = value.T
            slope[rs, at] = sig * (1.0 + pre * (1.0 - sig))

    def residual(rs):
        @pl.loop(0, tiles)
        def _(t):
            at = column(t)
            value = (rows[rs, at].astype(F32) + dot_nn(hid[rs, :], wide[1, :, at])).astype(BF16)
            resid[rs, at] = value
            resid_t[at, rs] = value.T

    for b, rs in enumerate(blocks):
        if b == len(blocks) - 1:
            forward(2, 2)
        arrive(row_swap[b])
        activate(rs)
        if b == 0:
            forward(1, 1)
            gathered(1)
        residual(rs)
    gathered(2)

    def classify(t, energy):
        at = column(t)
        logits = dot_nn(resid[...], wide[2, :, at])
        out = []
        for k in range(TILE // LANES):
            target = (lab_t[...] == lane + (t * TILE + k * LANES)).astype(F32)
            err = logits[:, k * LANES : (k + 1) * LANES] - target
            energy = energy + fold(err * err)
            out.append((err * norm).astype(BF16))
        dlog[:, at] = jnp.concatenate(out, axis=1)
        return energy

    def product(m, left_t, right, at):
        half = depth // 2

        @pl.loop(0, 2)
        def _(r):
            of = pl.ds(pl.multiple_of(r * half, half), half)
            grad[m, of, at] = dot_nn(left_t[of, :], right[:, at]).astype(BF16)

    to_core, to_pair, to_home = {}, {}, {}

    def scatter(key, m, at):
        to_core[key] = [
            begin(remote(piece(grad, m, 2 * q + 1 - core, at), from_core.at[m, q, :, at], twin))
            for q in range(pairs)
        ]
        to_pair[key] = []
        for d in range(1, pairs):
            q = pair_at(d)
            held = piece(grad, m, 2 * q + core, at)
            to_pair[key].append(remote(held, from_pair.at[m, d - 1, :, at], (ci, 2 * q + side)))
        started.extend(to_pair[key])
        held = piece(grad, m, 2 * pair + core, at)
        to_home[key] = swap(held, last.at[m, :, at])

    def combine(m, into, index, terms, at):
        @pl.loop(0, block // step)
        def _(r):
            off = pl.multiple_of(r * step, step)
            of = pl.ds(pl.multiple_of(index * block + off, step), step)
            total = grad[m, of, at].astype(F32)
            for term in terms:
                total = total + term[pl.ds(off, step), :].astype(F32)
            into[pl.ds(off, step), :] = total.astype(BF16)

    def scatter_on(key, m, at):
        for copy in to_core[key]:
            copy.wait_recv()
        for d in range(1, pairs):
            q = pair_at(d)
            held = piece(grad, m, 2 * q + core, at)
            combine(m, held, 2 * q + core, [from_core.at[m, q, :, at]], at)
            to_pair[key][d - 1].start()

    def scatter_home(key, m, at):
        for copy in to_pair[key]:
            copy.wait_recv()
        terms = [from_core.at[m, pair, :, at]]
        terms += [from_pair.at[m, d, :, at] for d in range(pairs - 1)]

        @pl.when(leads)
        def _():
            combine(m, last.at[m, :, at], 2 * pair + core, terms, at)

        @pl.when(moves)
        def _():
            combine(m, piece(grad, m, 2 * pair + core, at), 2 * pair + core, terms, at)
            to_home[key].start()

    def moved_on(key, m, at):
        @pl.when(moves)
        def _():
            scatter_on(key, m, at)

    def led_on(key, m, at):
        @pl.when(leads)
        def _():
            scatter_on(key, m, at)

    energy = zero
    for t in range(tiles):
        energy = classify(t, energy)
        product(2, resid_t, dlog, cols(t))
        scatter((2, t), 2, cols(t))
        if t > 0:
            moved_on((2, t - 1), 2, cols(t - 1))

    power[0] = energy * (0.5 * norm)
    power_swap = swap(power.at[0], power.at[1])
    send(power_swap)
    for copy in sums_out:
        copy.wait_recv()

    def over_dp(ref, k):
        total = ref[0, k]
        for j in range(1, n):
            total = total + ref[j, k]
        return whole(total)

    sq_ahead, sq_behind, mixed = (over_dp(sums, k) for k in range(3))
    len_ahead = jnp.sqrt(sq_ahead + EPS)
    len_behind = jnp.sqrt(sq_behind + EPS)
    raw_sq = (
        sq_ahead / (len_ahead * len_ahead)
        + sq_behind / (len_behind * len_behind)
        + 2.0 * mixed / (len_ahead * len_behind)
    )
    raw_len = jnp.sqrt(raw_sq + EPS)
    spans[ci, 0] = jnp.broadcast_to(len_behind, (8, LANES))
    spans[ci, 1] = jnp.broadcast_to(len_ahead, (8, LANES))
    spans_out = [
        begin(remote(spans.at[ci], spans.at[ci], (lax.rem(ci + d, c), me))) for d in range(1, c)
    ]
    by_ahead = 1.0 / (len_ahead * raw_len)
    by_behind = 1.0 / (len_behind * raw_len)

    for t in range(tiles):
        at = cols(t)
        dres[:, at] = dot_nt(dlog[...], wide[2, at, :]).astype(BF16)
        if t == 0:
            moved_on((2, tiles - 1), 2, cols(tiles - 1))
        led_on((2, t), 2, at)
        product(1, hid_t, dres, at)
        scatter((1, t), 1, at)
        if t > 0:
            scatter_on((1, t - 1), 1, cols(t - 1))
    @pl.loop(0, tiles)
    def _(t):
        at = column(t)
        rows_t[at, :] = rows[:, at].T
    scatter_on((1, tiles - 1), 1, cols(tiles - 1))

    for t in range(tiles):
        at = cols(t)
        dlog[:, at] = (dot_nt(dres[...], wide[1, at, :]) * slope[:, at]).astype(BF16)
        product(0, rows_t, dlog, at)
        scatter((0, t), 0, at)
        if t > 0:
            scatter_on((0, t - 1), 0, cols(t - 1))

        @pl.when(moves)
        def _():
            scatter_home((2, t), 2, at)
    for m in range(3):

        def body(r, _, m=m):
            at = pl.ds(pl.multiple_of(r * step, step), step)
            ahead, behind = differences(m, at)
            tau[m][at, :] = ahead * by_ahead + behind * by_behind
            return 0

        lax.fori_loop(0, block // step, body, 0)
    scatter_on((0, tiles - 1), 0, cols(tiles - 1))

    @pl.when(leads)
    def _():
        for t in range(tiles):
            scatter_home((2, t), 2, cols(t))
    for copy in spans_out:
        copy.wait_recv()
    arc = jnp.zeros((1, 1), F32)
    band = jnp.zeros((1, 1), F32)
    for k in range(c):
        length = spans[k, 0, 0:1, 0:1]
        arc = arc + jnp.where(k <= ci, length, 0.0)
        band = band + length
    band = band + spans[c - 1, 1, 0:1, 0:1]
    arrive(power_swap)

    def finish(key, m, cs, carry):
        arrive(to_home[key])

        def body(r, carry):
            at = pl.ds(pl.multiple_of(r * step, step), step)
            total = last[m, at, cs].astype(F32) * factor[m]
            edge[m, at, cs] = total
            return carry[0] + fold(total * tau[m][at, cs]), carry[1] + fold(total * total)

        return lax.fori_loop(0, block // step, body, carry)

    carry = (zero, zero)
    for t in range(tiles):
        scatter_home((1, t), 1, cols(t))
    for i in range(tiles):
        carry = finish((2, i), 2, cols(i), carry)
        scatter_home((0, i), 0, cols(i))
    for m in (1, 0):
        for t in range(tiles):
            carry = finish((m, t), m, cols(t), carry)
    late[me, 0] = carry[0]
    late[me, 1] = carry[1]
    late[me, 2] = jnp.where(leads, power[0], power[1])
    late_out = [
        begin(remote(late.at[me], late.at[me], (ci, lax.rem(me + d, n)))) for d in range(1, n)
    ]
    for copy in late_out:
        copy.wait_recv()
    along, g_g, energy_all = (over_dp(late, k) for k in range(3))

    goal = (ci + 1).astype(F32) / (c + 1) * band
    coef = jnp.where(jnp.full((1, 1), climb[0]) == 1, 2.0 * along, along + SPRING * (goal - arc) / band)
    tau_sq = raw_sq / (raw_sq + EPS)
    force_sq = g_g - 2.0 * coef * along + coef * coef * tau_sq
    scale = band / (c + 1) / jnp.sqrt(force_sq + EPS)
    push = scale * coef
    def small(value):
        return jnp.broadcast_to(value, (1, LANES))

    o_small[0:1, :] = small(energy_all)
    o_small[1:2, :] = small(arc / band)
    o_small[2:3, :] = small(0.5 * raw_len)
    @pl.loop(0, classes // LANES)
    def _(k):
        at = pl.ds(pl.multiple_of(k * LANES, LANES), LANES)
        new = own[2, :, at] + (push * tau_out[:, at] - scale * edge[2, :, at])
        o_out[0, at, :] = new.T

    rest = classes % LANES
    if rest:
        low = classes - rest
        at = pl.ds(low, LANES)
        new = own[2, :, at] + (push * tau_out[:, at] - scale * edge[2, :, at])
        o_out[0, low:classes, :] = new.T[0:rest, :]
    for m in range(2):

        @pl.loop(0, block // step)
        def _(r):
            at = pl.ds(pl.multiple_of(r * step, step), step)
            tau[m][at, :] = own[m, at, :] + (push * tau[m][at, :] - scale * edge[m, at, :])
    @pl.when(has_next)
    def _():
        for copy in ups:
            copy.wait_send()

    @pl.when(has_prev)
    def _():
        for copy in downs:
            copy.wait_send()

    @pl.when(moves)
    def _():
        for copy in swapped:
            copy.wait_send()

    for copy in started:
        copy.wait_send()


def on_device(
    n,
    c,
    images_in,
    images_mid,
    images_out,
    ends_in,
    ends_mid,
    ends_out,
    data_pool,
    batch_rows,
    labels,
    climbing,
):
    block, width = images_in.shape[1], images_in.shape[2]
    classes = images_out.shape[2]
    depth = n * block
    batch = batch_rows.shape[1]
    pairs = n // 2
    copies = copies_of(n, c, width // TILE, 3)
    vmem = pl.BlockSpec(memory_space=pltpu.VMEM)
    anywhere = pl.BlockSpec(memory_space=pl.ANY)
    scalar = pl.BlockSpec(memory_space=pltpu.SMEM)
    outs = pl.pallas_call(
        functools.partial(kernel, n, c, classes),
        out_shape=(
            pltpu.VMEM(images_in.shape, F32),
            pltpu.VMEM(images_mid.shape, F32),
            pltpu.VMEM((1, classes, block), F32),
            pltpu.VMEM((8, LANES), F32),
        ),
        in_specs=[anywhere] * 7 + [vmem] * 2 + [scalar],
        out_specs=[vmem] * 4,
        scratch_shapes=[
            pltpu.VMEM((3, block, width), F32),
            pltpu.VMEM((3, block, width), F32),
            pltpu.VMEM((2, width, block), F32),
            pltpu.VMEM((block, width), F32),
            pltpu.VMEM((3, depth, width), BF16),
            pltpu.VMEM((3, block, width), BF16),
            pltpu.VMEM((3, block, width), BF16),
            pltpu.VMEM((3, block, width), BF16),
            pltpu.VMEM((3, block, width), BF16),
            pltpu.VMEM(data_pool.shape, BF16),
            pltpu.VMEM((batch, LANES), jnp.int32),
            pltpu.VMEM((8, batch), jnp.int32),
            pltpu.VMEM((8, batch), jnp.int32),
            pltpu.VMEM((batch, depth), BF16),
            pltpu.VMEM((batch, depth), BF16),
            pltpu.VMEM((batch, width), F32),
            pltpu.VMEM((batch, width), BF16),
            pltpu.VMEM((batch, depth), BF16),
            pltpu.VMEM((depth, batch), BF16),
            pltpu.VMEM((width, batch), BF16),
            pltpu.VMEM((depth, batch), BF16),
            pltpu.VMEM((batch, width), BF16),
            pltpu.VMEM((batch, depth), BF16),
            pltpu.VMEM((3, depth, width), BF16),
            pltpu.VMEM((3, pairs, block, width), BF16),
            pltpu.VMEM((3, max(pairs - 1, 1), block, width), BF16),
            pltpu.VMEM((3, block, width), BF16),
            pltpu.VMEM((2, 8, LANES), F32),
            pltpu.VMEM((n, 3, 8, LANES), F32),
            pltpu.VMEM((c, 2, 8, LANES), F32),
            pltpu.VMEM((n, 3, 8, LANES), F32),
            pltpu.SemaphoreType.DMA((7,)),
            pltpu.SemaphoreType.DMA((copies,)),
            pltpu.SemaphoreType.DMA((copies,)),
        ],
        compiler_params=pltpu.CompilerParams(
            collective_id=0, has_side_effects=True, vmem_limit_bytes=60 * 1024 * 1024
        ),
    )(
        images_in,
        images_mid,
        jnp.swapaxes(images_out, 1, 2),
        ends_in,
        ends_mid,
        jnp.swapaxes(ends_out, 1, 2),
        data_pool,
        batch_rows,
        labels,
        climbing,
    )
    return (outs[0], outs[1], jnp.swapaxes(outs[2], 1, 2), *(outs[3][k, 0:1] for k in range(3)))


def solution(mesh):
    placed = (
        P("chain", "dp", None),
        P("chain", "dp", None),
        P("chain", "dp", None),
        P(None, "dp", None),
        P(None, "dp", None),
        P(None, "dp", None),
        P("dp", None),
        P("chain", "dp"),
        P("chain", "dp"),
        P("chain"),
    )
    return jax.shard_map(
        functools.partial(on_device, mesh.shape["dp"], mesh.shape["chain"]),
        mesh=mesh,
        in_specs=placed,
        out_specs=(
            P("chain", "dp", None),
            P("chain", "dp", None),
            P("chain", "dp", None),
            P("chain"),
            P("chain"),
            P("chain"),
        ),
        check_vma=False,
    )
```

```python
import functools

import jax
import jax.numpy as jnp
from jax import lax
from jax.experimental import pallas as pl
from jax.experimental.pallas import tpu as pltpu
from jax.sharding import PartitionSpec as P

SPRING = 0.03
EPS = 1e-06
TILE = 256
LANES = 128
F32 = jnp.float32
BF16 = jnp.bfloat16


def copies_of(count, chain, chunks, rows):
    pairs = count // 2
    gather = 3 * (1 + (pairs - 1) + pairs)
    scatter = 3 * chunks * (pairs + (pairs - 1) + 1)
    return gather + scatter + 6 + 2 * (count - 1) + (chain - 1) + 2 + rows + chain // 2


def dot_nn(left, right):
    return jnp.dot(left, right, preferred_element_type=F32)


def dot_nt(left, right):
    return lax.dot_general(left, right, (((1,), (1,)), ((), ())), preferred_element_type=F32)


def dot_tn(left, right):
    return lax.dot_general(left, right, (((0,), (0,)), ((), ())), preferred_element_type=F32)


def fold(value):
    part = jnp.sum(value.reshape(value.shape[0] // 8, 8, value.shape[1]), axis=0)
    total = part[:, :LANES]
    for k in range(1, value.shape[1] // LANES):
        total = total + part[:, k * LANES : (k + 1) * LANES]
    return total


def whole(tile):
    return jnp.sum(tile, axis=(0, 1), keepdims=True)


def kernel(
    n,
    c,
    classes,
    p_in,
    p_mid,
    p_out,
    e_in,
    e_mid,
    e_out,
    pool,
    picks,
    labs,
    climb,
    o_in,
    o_mid,
    o_out,
    o_small,
    own,
    edge,
    thin,
    tau_out,
    wide,
    stage,
    near,
    before,
    after,
    pool_v,
    pool_x,
    lab_t,
    lab_out,
    lab_in,
    rows_out,
    rows,
    slope,
    hid,
    resid,
    rows_t,
    hid_t,
    resid_t,
    dlog,
    dres,
    grad,
    from_core,
    from_pair,
    last,
    power,
    sums,
    spans,
    late,
    load_sem,
    send_sem,
    recv_sem,
):
    ci, me = lax.axis_index("chain"), lax.axis_index("dp")
    pairs = n // 2
    core, side = lax.rem(ci, 2), lax.rem(me, 2)
    pair = me // 2
    leads = core == side
    moves = core != side
    cross = (ci + 1 - 2 * core, me + 1 - 2 * side)
    twin = (ci + 1 - 2 * core, me)
    block, width = own.shape[1], own.shape[2]
    depth = n * block
    step = min(32, block)
    batch = rows.shape[0]
    tiles = width // TILE
    factor = (depth**-0.5, width**-0.5, depth**-0.5)
    norm = 1.0 / (batch * n * classes)
    counter = [0]
    tau = [o_in.at[0], o_mid.at[0], tau_out]

    def remote(src, dst, to):
        k = counter[0]
        counter[0] += 1
        copy = pltpu.make_async_remote_copy(
            src_ref=src,
            dst_ref=dst,
            send_sem=send_sem.at[k],
            recv_sem=recv_sem.at[k],
            device_id=to,
            device_id_type=pl.DeviceIdType.MESH,
        )
        return copy

    def pair_at(d):
        return lax.rem(pair + d, pairs)
    barrier = pltpu.get_barrier_semaphore()
    for d in range(1, n):
        pl.semaphore_signal(
            barrier, inc=1, device_id=(ci, lax.rem(me + d, n)), device_id_type=pl.DeviceIdType.MESH
        )
    for d in range(1, c):
        pl.semaphore_signal(
            barrier, inc=1, device_id=(lax.rem(ci + d, c), me), device_id_type=pl.DeviceIdType.MESH
        )

    pl.semaphore_signal(barrier, inc=1, device_id=cross, device_id_type=pl.DeviceIdType.MESH)

    end = jnp.where(ci == 0, 0, 1)
    loads = [
        pltpu.make_async_copy(p_in.at[0], own.at[0], load_sem.at[0]),
        pltpu.make_async_copy(p_mid.at[0], own.at[1], load_sem.at[1]),
        pltpu.make_async_copy(p_out.at[0], thin.at[0, pl.ds(0, classes)], load_sem.at[2]),
        pltpu.make_async_copy(pool, pool_v, load_sem.at[3]),
        pltpu.make_async_copy(e_in.at[end], edge.at[0], load_sem.at[4]),
        pltpu.make_async_copy(e_mid.at[end], edge.at[1], load_sem.at[5]),
        pltpu.make_async_copy(e_out.at[end], thin.at[1, pl.ds(0, classes)], load_sem.at[6]),
    ]
    for k in (0, 3, 1, 2, 4, 5, 6):
        loads[k].start()

    def turned(into, thin_at):
        @pl.loop(0, width // LANES)
        def _(k):
            at = pl.ds(pl.multiple_of(k * LANES, LANES), LANES)
            into[:, at] = thin[thin_at, at, :].T

    def blanked(thin_at):
        if classes < width:
            thin[thin_at, pl.ds(classes, width - classes), :] = jnp.zeros(
                (width - classes, block), F32
            )

    def lowered(m):
        def body(r, _):
            off = pl.multiple_of(r * step, step)
            value = own[m, pl.ds(off, step), :]
            low = (value * factor[m]).astype(BF16)
            stage[m, pl.ds(off, step), :] = low

            @pl.when(leads)
            def _():
                wide[m, pl.ds(pl.multiple_of(me * block + off, step), step), :] = low

            near[m, pl.ds(off, step), :] = value.astype(BF16)
            return 0

        lax.fori_loop(0, block // step, body, 0)

    def column(t):
        return pl.ds(pl.multiple_of(t * TILE, TILE), TILE)

    everything, everyone = pl.ds(0, width), pl.ds(0, batch)
    cuts = [0] + [at for at in (batch - 2 * TILE, batch - TILE) if at > 0] + [batch]
    blocks = [pl.ds(low, high - low) for low, high in zip(cuts[:-1], cuts[1:])]

    def piece(ref, m, index, at=everything):
        return ref.at[m, pl.ds(pl.multiple_of(index * block, block), block), at]

    started = []

    def begin(copy):
        copy.start()
        started.append(copy)
        return copy

    hop, across, over = {}, {}, {}
    swapped = []

    def swap(src, dst):
        copy = remote(src, dst, cross)
        swapped.append(copy)
        return copy

    def send(*copies):
        @pl.when(moves)
        def _():
            for copy in copies:
                copy.start()

    def arrive(*copies):
        @pl.when(moves)
        def _():
            for copy in copies:
                copy.wait_recv()

    def prepare(key, m, at=everything):
        hop[key] = swap(stage.at[m, :, at], piece(wide, m, me, at))
        held = piece(wide, m, 2 * pair + core, at)
        across[key] = [
            remote(held, held, (ci, 2 * pair_at(d) + side)) for d in range(1, pairs)
        ]
        over[key] = [remote(held, held, twin)]
        started.extend(across[key] + over[key])

    def spread(key):
        for copy in across[key] + over[key][:1]:
            copy.start()

    def spread_own(*keys):
        @pl.when(leads)
        def _():
            for key in keys:
                spread(key)

    def spread_moved(*keys):
        @pl.when(moves)
        def _():
            for key in keys:
                hop[key].wait_recv()
                spread(key)

    def forward(key, m, at=everything):
        for d in range(1, pairs):
            across[key][d - 1].wait_recv()
            held = piece(wide, m, 2 * pair_at(pairs - d) + core, at)
            over[key].append(begin(remote(held, held, twin)))

    def gathered(key):
        for copy in over[key]:
            copy.wait_recv()

    def cols(t):
        return pl.ds(t * TILE, TILE)

    for m in range(3):
        prepare(m, m)
    loads[0].wait()
    lowered(0)
    pl.semaphore_wait(barrier, n - 1 + c - 1 + 1)
    planes, plane = c // 2, ci // 2
    share = pool_v.shape[0] // planes
    mine = pl.ds(pl.multiple_of(plane * share, share), share)
    beyond = pl.ds(width - pool_x.shape[1], pool_x.shape[1])
    pool_swap = swap(pool_v.at[mine, beyond], pool_x.at[mine])
    pool_out = [
        remote(pool_x.at[mine], pool_x.at[mine], (lax.rem(ci + 2 * d, c), me))
        for d in range(1, planes)
    ]
    loads[3].wait()
    send(pool_swap, hop[0])
    spread_own(0)
    loads[1].wait()
    lowered(1)
    send(hop[1])
    spread_own(1)
    blanked(0)
    blanked(1)
    loads[2].wait()
    turned(own.at[2], 0)
    lowered(2)
    send(hop[2])
    spread_own(2)
    lab_out[0] = jnp.broadcast_to(labs[...], (8, batch))
    lab_out[1] = jnp.broadcast_to(picks[...], (8, batch))

    @pl.when(leads)
    def _():
        lab_in[0] = lab_out[0]

    lab_swap = swap(lab_out, lab_in)
    send(lab_swap)
    lane = lax.broadcasted_iota(jnp.int32, (batch, LANES), 1)
    supply = pool_v.shape[0]
    reach = [(m, min(width, supply - m * width)) for m in range(-(-supply // width))]

    def choose(row_of):
        for k in range(supply // LANES):
            m, at = k * LANES // width, k * LANES % width
            grad[m, 0:batch, at : at + LANES] = (
                (row_of == lane + k * LANES).astype(F32).astype(BF16)
            )

    def picked_of(rs, source, at):
        return sum(
            dot_nn(grad[m, rs, 0:size], source[pl.ds(m * width, size), at]) for m, size in reach
        ).astype(BF16)

    choose(jnp.broadcast_to(picks[...], (LANES, batch)).T)
    direct = width - pool_x.shape[1]
    row_swap = []
    for rs in blocks:
        for k in range(direct // TILE):
            picked = picked_of(rs, pool_v, cols(k))
            rows_out[rs, cols(k)] = picked

            @pl.when(leads)
            def _():
                rows[rs, cols(k)] = picked

        row_swap.append(swap(rows_out.at[rs, 0:direct], rows.at[rs, 0:direct]))
        send(row_swap[-1])
    @pl.when(leads)
    def _():
        for k in range(direct // TILE, tiles):
            rows[:, cols(k)] = picked_of(everyone, pool_v, cols(k))

    @pl.when(moves)
    def _():
        pool_swap.wait_recv()

        @pl.when(plane < planes // 2)
        def _():
            for copy in pool_out[::-1]:
                copy.start()

        @pl.when(plane >= planes // 2)
        def _():
            for copy in pool_out:
                copy.start()
    spread_moved(0, 1, 2)
    forward(0, 0)
    for load in loads[4:]:
        load.wait()
    turned(edge.at[2], 1)

    def differences(m, at):
        mine = own[m, at, :]
        fixed = edge[m, at, :]
        left = jnp.where(ci == 0, fixed, before[m, at, :].astype(F32))
        right = jnp.where(ci == c - 1, fixed, after[m, at, :].astype(F32))
        return right - mine, mine - left

    zero = jnp.zeros((8, LANES), F32)
    arrive(lab_swap)
    lab_t[...] = jnp.broadcast_to(lab_in[0][0:1, :], (LANES, batch)).T
    @pl.when(moves)
    def _():
        choose(jnp.broadcast_to(lab_in[1][0:1, :], (LANES, batch)).T)
        for copy in pool_out:
            copy.wait_recv()
    @pl.when(moves)
    def _():
        for k in range(direct // TILE, tiles):
            rows[:, cols(k)] = picked_of(everyone, pool_x, cols(k - direct // TILE))
    gathered(0)

    def activate(rs):
        for t in range(tiles):
            at = cols(t)
            pre = dot_nn(rows[rs, :], wide[0, :, at])
            sig = jax.nn.sigmoid(pre)
            value = (pre * sig).astype(BF16)
            hid[rs, at] = value
            hid_t[at, rs] = value.T
            slope[rs, at] = sig * (1.0 + pre * (1.0 - sig))

    def residual(rs):
        for t in range(tiles):
            at = cols(t)
            value = (rows[rs, at].astype(F32) + dot_nn(hid[rs, :], wide[1, :, at])).astype(BF16)
            resid[rs, at] = value
            resid_t[at, rs] = value.T

    ups = [remote(near.at[m], before.at[m], (lax.rem(ci + 1, c), me)) for m in range(3)]
    downs = [remote(near.at[m], after.at[m], (lax.rem(ci + c - 1, c), me)) for m in range(3)]
    has_next, has_prev = ci < c - 1, ci > 0

    for b, rs in enumerate(blocks):
        arrive(row_swap[b])
        activate(rs)
        if b == 0:
            forward(1, 1)
            gathered(1)
            @pl.when(has_next)
            def _():
                for copy in ups:
                    copy.start()

            @pl.when(has_prev)
            def _():
                for copy in downs:
                    copy.start()

        if b == len(blocks) - 1:
            forward(2, 2)
        residual(rs)
    gathered(2)

    def classify(t, energy):
        at = column(t)
        logits = dot_nn(resid[...], wide[2, :, at])
        out = []
        for k in range(TILE // LANES):
            target = (lab_t[...] == lane + (t * TILE + k * LANES)).astype(F32)
            err = logits[:, k * LANES : (k + 1) * LANES] - target
            energy = energy + fold(err * err)
            out.append((err * norm).astype(BF16))
        dlog[:, at] = jnp.concatenate(out, axis=1)
        return energy

    def product(m, left_t, right, at):
        half = depth // 2

        @pl.loop(0, 2)
        def _(r):
            of = pl.ds(pl.multiple_of(r * half, half), half)
            grad[m, of, at] = dot_nn(left_t[of, :], right[:, at]).astype(BF16)

    to_core, to_pair, to_home = {}, {}, {}

    def scatter(key, m, at):
        to_core[key] = [
            begin(remote(piece(grad, m, 2 * q + 1 - core, at), from_core.at[m, q, :, at], twin))
            for q in range(pairs)
        ]
        to_pair[key] = []
        for d in range(1, pairs):
            q = pair_at(d)
            held = piece(grad, m, 2 * q + core, at)
            to_pair[key].append(remote(held, from_pair.at[m, d - 1, :, at], (ci, 2 * q + side)))
        started.extend(to_pair[key])
        held = piece(grad, m, 2 * pair + core, at)
        to_home[key] = swap(held, last.at[m, :, at])

    def combine(m, into, index, terms, at):
        @pl.loop(0, block // step)
        def _(r):
            off = pl.multiple_of(r * step, step)
            of = pl.ds(pl.multiple_of(index * block + off, step), step)
            total = grad[m, of, at].astype(F32)
            for term in terms:
                total = total + term[pl.ds(off, step), :].astype(F32)
            into[pl.ds(off, step), :] = total.astype(BF16)

    def scatter_on(key, m, at):
        for copy in to_core[key]:
            copy.wait_recv()
        for d in range(1, pairs):
            q = pair_at(d)
            held = piece(grad, m, 2 * q + core, at)
            combine(m, held, 2 * q + core, [from_core.at[m, q, :, at]], at)
            to_pair[key][d - 1].start()

    def scatter_home(key, m, at):
        for copy in to_pair[key]:
            copy.wait_recv()
        terms = [from_core.at[m, pair, :, at]]
        terms += [from_pair.at[m, d, :, at] for d in range(pairs - 1)]

        @pl.when(leads)
        def _():
            combine(m, last.at[m, :, at], 2 * pair + core, terms, at)

        @pl.when(moves)
        def _():
            combine(m, piece(grad, m, 2 * pair + core, at), 2 * pair + core, terms, at)
            to_home[key].start()

    def moved_on(key, m, at):
        @pl.when(moves)
        def _():
            scatter_on(key, m, at)

    def led_on(key, m, at):
        @pl.when(leads)
        def _():
            scatter_on(key, m, at)

    energy = zero
    for t in range(tiles):
        energy = classify(t, energy)
        product(2, resid_t, dlog, cols(t))
        scatter((2, t), 2, cols(t))
        if t > 0:
            moved_on((2, t - 1), 2, cols(t - 1))

    power[0] = energy * (0.5 * norm)
    power_swap = swap(power.at[0], power.at[1])
    send(power_swap)

    for t in range(tiles):
        at = cols(t)
        dres[:, at] = dot_nt(dlog[...], wide[2, at, :]).astype(BF16)
        if t == 0:
            moved_on((2, tiles - 1), 2, cols(tiles - 1))
        led_on((2, t), 2, at)
        product(1, hid_t, dres, at)
        scatter((1, t), 1, at)
        if t > 0:
            scatter_on((1, t - 1), 1, cols(t - 1))
    @pl.when(has_prev)
    def _():
        for copy in ups:
            copy.wait_recv()

    @pl.when(has_next)
    def _():
        for copy in downs:
            copy.wait_recv()

    def span_sums(m, carry):
        def body(r, carry):
            ahead, behind = differences(m, pl.ds(pl.multiple_of(r * step, step), step))
            return (
                carry[0] + fold(ahead * ahead),
                carry[1] + fold(behind * behind),
                carry[2] + fold(ahead * behind),
            )

        return lax.fori_loop(0, block // step, body, carry)

    carry = (zero, zero, zero)
    for m in range(3):
        carry = span_sums(m, carry)
    for k in range(3):
        sums[me, k] = carry[k]
    sums_out = [
        begin(remote(sums.at[me], sums.at[me], (ci, lax.rem(me + d, n)))) for d in range(1, n)
    ]
    @pl.loop(0, tiles)
    def _(t):
        at = column(t)
        rows_t[at, :] = rows[:, at].T
    scatter_on((1, tiles - 1), 1, cols(tiles - 1))

    for t in range(tiles):
        at = cols(t)
        dlog[:, at] = (dot_nt(dres[...], wide[1, at, :]) * slope[:, at]).astype(BF16)
        product(0, rows_t, dlog, at)
        scatter((0, t), 0, at)
        if t > 0:
            scatter_on((0, t - 1), 0, cols(t - 1))

        @pl.when(moves)
        def _():
            scatter_home((2, t), 2, at)
    scatter_on((0, tiles - 1), 0, cols(tiles - 1))

    @pl.when(leads)
    def _():
        for t in range(tiles):
            scatter_home((2, t), 2, cols(t))

    def finish(key, m, cs, carry):
        arrive(to_home[key])

        def body(r, carry):
            at = pl.ds(pl.multiple_of(r * step, step), step)
            total = last[m, at, cs].astype(F32) * factor[m]
            edge[m, at, cs] = total
            return carry[0] + fold(total * tau[m][at, cs]), carry[1] + fold(total * total)

        return lax.fori_loop(0, block // step, body, carry)

    carry = (zero, zero)
    for t in range(tiles):
        scatter_home((1, t), 1, cols(t))
    for copy in sums_out:
        copy.wait_recv()

    def over_dp(ref, k):
        total = ref[0, k]
        for j in range(1, n):
            total = total + ref[j, k]
        return whole(total)

    sq_ahead, sq_behind, mixed = (over_dp(sums, k) for k in range(3))
    len_ahead = jnp.sqrt(sq_ahead + EPS)
    len_behind = jnp.sqrt(sq_behind + EPS)
    raw_sq = (
        sq_ahead / (len_ahead * len_ahead)
        + sq_behind / (len_behind * len_behind)
        + 2.0 * mixed / (len_ahead * len_behind)
    )
    raw_len = jnp.sqrt(raw_sq + EPS)
    spans[ci, 0] = jnp.broadcast_to(len_behind, (8, LANES))
    spans[ci, 1] = jnp.broadcast_to(len_ahead, (8, LANES))
    spans_out = [
        begin(remote(spans.at[ci], spans.at[ci], (lax.rem(ci + d, c), me))) for d in range(1, c)
    ]
    by_ahead = 1.0 / (len_ahead * raw_len)
    by_behind = 1.0 / (len_behind * raw_len)
    for m in range(3):

        def body(r, _, m=m):
            at = pl.ds(pl.multiple_of(r * step, step), step)
            ahead, behind = differences(m, at)
            tau[m][at, :] = ahead * by_ahead + behind * by_behind
            return 0

        lax.fori_loop(0, block // step, body, 0)

    for i in range(tiles):
        carry = finish((2, i), 2, cols(i), carry)
        scatter_home((0, i), 0, cols(i))
    for m in (1, 0):
        for t in range(tiles):
            carry = finish((m, t), m, cols(t), carry)
    arrive(power_swap)
    late[me, 0] = carry[0]
    late[me, 1] = carry[1]
    late[me, 2] = jnp.where(leads, power[0], power[1])
    late_out = [
        begin(remote(late.at[me], late.at[me], (ci, lax.rem(me + d, n)))) for d in range(1, n)
    ]
    for copy in spans_out:
        copy.wait_recv()
    arc = jnp.zeros((1, 1), F32)
    band = jnp.zeros((1, 1), F32)
    for k in range(c):
        length = spans[k, 0, 0:1, 0:1]
        arc = arc + jnp.where(k <= ci, length, 0.0)
        band = band + length
    band = band + spans[c - 1, 1, 0:1, 0:1]
    for copy in late_out:
        copy.wait_recv()
    along, g_g, energy_all = (over_dp(late, k) for k in range(3))

    goal = (ci + 1).astype(F32) / (c + 1) * band
    coef = jnp.where(jnp.full((1, 1), climb[0]) == 1, 2.0 * along, along + SPRING * (goal - arc) / band)
    tau_sq = raw_sq / (raw_sq + EPS)
    force_sq = g_g - 2.0 * coef * along + coef * coef * tau_sq
    scale = band / (c + 1) / jnp.sqrt(force_sq + EPS)
    push = scale * coef
    def small(value):
        return jnp.broadcast_to(value, (1, LANES))

    o_small[0:1, :] = small(energy_all)
    o_small[1:2, :] = small(arc / band)
    o_small[2:3, :] = small(0.5 * raw_len)
    @pl.loop(0, classes // LANES)
    def _(k):
        at = pl.ds(pl.multiple_of(k * LANES, LANES), LANES)
        new = own[2, :, at] + (push * tau_out[:, at] - scale * edge[2, :, at])
        o_out[0, at, :] = new.T

    rest = classes % LANES
    if rest:
        low = classes - rest
        at = pl.ds(low, LANES)
        new = own[2, :, at] + (push * tau_out[:, at] - scale * edge[2, :, at])
        o_out[0, low:classes, :] = new.T[0:rest, :]
    for m in range(2):

        @pl.loop(0, block // step)
        def _(r):
            at = pl.ds(pl.multiple_of(r * step, step), step)
            tau[m][at, :] = own[m, at, :] + (push * tau[m][at, :] - scale * edge[m, at, :])
    @pl.when(has_next)
    def _():
        for copy in ups:
            copy.wait_send()

    @pl.when(has_prev)
    def _():
        for copy in downs:
            copy.wait_send()

    @pl.when(moves)
    def _():
        for copy in swapped + pool_out:
            copy.wait_send()

    for copy in started:
        copy.wait_send()


def on_device(
    n,
    c,
    images_in,
    images_mid,
    images_out,
    ends_in,
    ends_mid,
    ends_out,
    data_pool,
    batch_rows,
    labels,
    climbing,
):
    block, width = images_in.shape[1], images_in.shape[2]
    classes = images_out.shape[2]
    depth = n * block
    batch = batch_rows.shape[1]
    pairs = n // 2
    copies = copies_of(n, c, width // TILE, 3)
    vmem = pl.BlockSpec(memory_space=pltpu.VMEM)
    anywhere = pl.BlockSpec(memory_space=pl.ANY)
    scalar = pl.BlockSpec(memory_space=pltpu.SMEM)
    outs = pl.pallas_call(
        functools.partial(kernel, n, c, classes),
        out_shape=(
            pltpu.VMEM(images_in.shape, F32),
            pltpu.VMEM(images_mid.shape, F32),
            pltpu.VMEM((1, classes, block), F32),
            pltpu.VMEM((8, LANES), F32),
        ),
        in_specs=[anywhere] * 7 + [vmem] * 2 + [scalar],
        out_specs=[vmem] * 4,
        scratch_shapes=[
            pltpu.VMEM((3, block, width), F32),
            pltpu.VMEM((3, block, width), F32),
            pltpu.VMEM((2, width, block), F32),
            pltpu.VMEM((block, width), F32),
            pltpu.VMEM((3, depth, width), BF16),
            pltpu.VMEM((3, block, width), BF16),
            pltpu.VMEM((3, block, width), BF16),
            pltpu.VMEM((3, block, width), BF16),
            pltpu.VMEM((3, block, width), BF16),
            pltpu.VMEM(data_pool.shape, BF16),
            pltpu.VMEM((data_pool.shape[0], width // 2), BF16),
            pltpu.VMEM((batch, LANES), jnp.int32),
            pltpu.VMEM((2, 8, batch), jnp.int32),
            pltpu.VMEM((2, 8, batch), jnp.int32),
            pltpu.VMEM((batch, depth), BF16),
            pltpu.VMEM((batch, depth), BF16),
            pltpu.VMEM((batch, width), F32),
            pltpu.VMEM((batch, width), BF16),
            pltpu.VMEM((batch, depth), BF16),
            pltpu.VMEM((depth, batch), BF16),
            pltpu.VMEM((width, batch), BF16),
            pltpu.VMEM((depth, batch), BF16),
            pltpu.VMEM((batch, width), BF16),
            pltpu.VMEM((batch, depth), BF16),
            pltpu.VMEM((3, depth, width), BF16),
            pltpu.VMEM((3, pairs, block, width), BF16),
            pltpu.VMEM((3, max(pairs - 1, 1), block, width), BF16),
            pltpu.VMEM((3, block, width), BF16),
            pltpu.VMEM((2, 8, LANES), F32),
            pltpu.VMEM((n, 3, 8, LANES), F32),
            pltpu.VMEM((c, 2, 8, LANES), F32),
            pltpu.VMEM((n, 3, 8, LANES), F32),
            pltpu.SemaphoreType.DMA((7,)),
            pltpu.SemaphoreType.DMA((copies,)),
            pltpu.SemaphoreType.DMA((copies,)),
        ],
        compiler_params=pltpu.CompilerParams(
            collective_id=0, has_side_effects=True, vmem_limit_bytes=60 * 1024 * 1024
        ),
    )(
        images_in,
        images_mid,
        jnp.swapaxes(images_out, 1, 2),
        ends_in,
        ends_mid,
        jnp.swapaxes(ends_out, 1, 2),
        data_pool,
        batch_rows,
        labels,
        climbing,
    )
    return (outs[0], outs[1], jnp.swapaxes(outs[2], 1, 2), *(outs[3][k, 0:1] for k in range(3)))


def solution(mesh):
    placed = (
        P("chain", "dp", None),
        P("chain", "dp", None),
        P("chain", "dp", None),
        P(None, "dp", None),
        P(None, "dp", None),
        P(None, "dp", None),
        P("dp", None),
        P("chain", "dp"),
        P("chain", "dp"),
        P("chain"),
    )
    return jax.shard_map(
        functools.partial(on_device, mesh.shape["dp"], mesh.shape["chain"]),
        mesh=mesh,
        in_specs=placed,
        out_specs=(
            P("chain", "dp", None),
            P("chain", "dp", None),
            P("chain", "dp", None),
            P("chain"),
            P("chain"),
            P("chain"),
        ),
        check_vma=False,
    )
```

```python
import functools

import jax
import jax.numpy as jnp
from jax import lax
from jax.experimental import pallas as pl
from jax.experimental.pallas import tpu as pltpu
from jax.sharding import PartitionSpec as P

SPRING = 0.03
EPS = 1e-06
TILE = 256
LANES = 128
F32 = jnp.float32
BF16 = jnp.bfloat16


def semaphores(count, chunks, rows):
    pairs = count // 2
    sends = 1 + (pairs - 1) + pairs + 2 + 5 + 3 + 1 + (pairs - 1) + 1 + 1
    receives = (2 + chunks) * ((pairs - 1) + pairs) + 3 + 2 + 4 + rows + 3 + 9 * chunks + 3 + 1
    return sends, receives


def dot_nn(left, right):
    return jnp.dot(left, right, preferred_element_type=F32)


def dot_nt(left, right):
    return lax.dot_general(left, right, (((1,), (1,)), ((), ())), preferred_element_type=F32)


def dot_tn(left, right):
    return lax.dot_general(left, right, (((0,), (0,)), ((), ())), preferred_element_type=F32)


def fold(value):
    part = jnp.sum(value.reshape(value.shape[0] // 8, 8, value.shape[1]), axis=0)
    total = part[:, :LANES]
    for k in range(1, value.shape[1] // LANES):
        total = total + part[:, k * LANES : (k + 1) * LANES]
    return total


def whole(tile):
    return jnp.sum(tile, axis=(0, 1), keepdims=True)


def kernel(
    n,
    c,
    classes,
    p_in,
    p_mid,
    p_out,
    e_in,
    e_mid,
    e_out,
    pool,
    picks,
    labs,
    climb,
    o_in,
    o_mid,
    o_out,
    o_small,
    own,
    edge,
    thin,
    tau_out,
    wide,
    stage,
    near,
    before,
    after,
    pool_v,
    pool_x,
    lab_t,
    lab_out,
    lab_in,
    rows_out,
    rows,
    slope,
    hid,
    resid,
    rows_t,
    hid_t,
    resid_t,
    dlog,
    dres,
    grad,
    from_core,
    from_pair,
    last,
    power,
    sums,
    spans,
    late,
    load_sem,
    send_sem,
    recv_sem,
):
    ci, me = lax.axis_index("chain"), lax.axis_index("dp")
    pairs = n // 2
    core, side = lax.rem(ci, 2), lax.rem(me, 2)
    pair = me // 2
    leads = core == side
    moves = core != side
    cross = (ci + 1 - 2 * core, me + 1 - 2 * side)
    twin = (ci + 1 - 2 * core, me)
    block, width = own.shape[1], own.shape[2]
    depth = n * block
    step = min(32, block)
    batch = rows.shape[0]
    tiles = width // TILE
    factor = (depth**-0.5, width**-0.5, depth**-0.5)
    norm = 1.0 / (batch * n * classes)
    counts = [0, 0]
    tau = [o_in.at[0], o_mid.at[0], tau_out]

    def ticket(kind):
        counts[kind] += 1
        return counts[kind] - 1

    def remote(src, dst, to, out=None, into=None):
        return pltpu.make_async_remote_copy(
            src_ref=src,
            dst_ref=dst,
            send_sem=send_sem.at[ticket(0) if out is None else out],
            recv_sem=recv_sem.at[ticket(1) if into is None else into],
            device_id=to,
            device_id_type=pl.DeviceIdType.MESH,
        )

    def sent(ref, out):
        remote(ref, ref, twin, out, 0).wait_send()

    def landed(ref, into):
        remote(ref, ref, twin, 0, into).wait_recv()

    def pair_at(d):
        return lax.rem(pair + d, pairs)
    barrier = pltpu.get_barrier_semaphore()
    for d in range(1, n):
        pl.semaphore_signal(
            barrier, inc=1, device_id=(ci, lax.rem(me + d, n)), device_id_type=pl.DeviceIdType.MESH
        )
    for d in range(1, c):
        pl.semaphore_signal(
            barrier, inc=1, device_id=(lax.rem(ci + d, c), me), device_id_type=pl.DeviceIdType.MESH
        )

    pl.semaphore_signal(barrier, inc=1, device_id=cross, device_id_type=pl.DeviceIdType.MESH)

    end = jnp.where(ci == 0, 0, 1)
    planes, plane = c // 2, ci // 2
    share = pool_v.shape[0] // planes
    mine = pl.ds(pl.multiple_of(plane * share, share), share)

    def load(k, src, dst):
        return pltpu.make_async_copy(src, dst, load_sem.at[k])

    def pool_rows(d):
        return pl.ds(pl.multiple_of(lax.rem(plane + d, planes) * share, share), share)

    loads = [
        load(0, p_in.at[0], own.at[0]),
        load(1, p_mid.at[0], own.at[1]),
        load(2, p_out.at[0], thin.at[0, pl.ds(0, classes)]),
        load(3, e_in.at[end], edge.at[0]),
        load(4, e_mid.at[end], edge.at[1]),
        load(5, e_out.at[end], thin.at[1, pl.ds(0, classes)]),
    ]
    pool_loads = [
        load(6 + d, pool.at[pool_rows(d)], pool_v.at[pool_rows(d)]) for d in range(planes)
    ]
    for copy in (
        [pool_loads[0], loads[0]] + loads[1:3] + pool_loads[1:] + loads[3:6]
    ):
        copy.start()

    def turned(into, thin_at):
        @pl.loop(0, width // LANES)
        def _(k):
            at = pl.ds(pl.multiple_of(k * LANES, LANES), LANES)
            into[:, at] = thin[thin_at, at, :].T

    def blanked(thin_at):
        if classes < width:
            thin[thin_at, pl.ds(classes, width - classes), :] = jnp.zeros(
                (width - classes, block), F32
            )

    def lowered(m):
        def body(r, _):
            off = pl.multiple_of(r * step, step)
            value = own[m, pl.ds(off, step), :]
            low = (value * factor[m]).astype(BF16)
            stage[m, pl.ds(off, step), :] = low

            @pl.when(leads)
            def _():
                wide[m, pl.ds(pl.multiple_of(me * block + off, step), step), :] = low

            near[m, pl.ds(off, step), :] = value.astype(BF16)
            return 0

        lax.fori_loop(0, block // step, body, 0)

    def column(t):
        return pl.ds(pl.multiple_of(t * TILE, TILE), TILE)

    everything, everyone = pl.ds(0, width), pl.ds(0, batch)
    cuts = [0] + [at for at in (batch - 4 * LANES, batch - LANES) if at > 0] + [batch]
    blocks = [pl.ds(low, high - low) for low, high in zip(cuts[:-1], cuts[1:])]

    def piece(ref, m, index, at=everything):
        return ref.at[m, pl.ds(pl.multiple_of(index * block, block), block), at]

    hop, across, over = {}, {}, {}
    def swap(src, dst, out=None):
        return remote(src, dst, cross, out)

    def send(*copies):
        @pl.when(moves)
        def _():
            for copy in copies:
                copy.start()

    def arrive(*copies):
        @pl.when(moves)
        def _():
            for copy in copies:
                copy.wait_recv()

    hop_out = ticket(0)
    across_out = [ticket(0) for _ in range(1, pairs)]
    over_out = [ticket(0) for _ in range(pairs)]

    def prepare(m):
        hop[m] = swap(stage.at[m], piece(wide, m, me), hop_out)
        held = piece(wide, m, 2 * pair + core)
        across[m] = [
            remote(held, held, (ci, 2 * pair_at(d) + side), across_out[d - 1])
            for d in range(1, pairs)
        ]
        over[m] = [remote(held, held, twin, over_out[0])]
        for d in range(1, pairs):
            held = piece(wide, m, 2 * pair_at(pairs - d) + core)
            over[m].append(remote(held, held, twin, over_out[d]))

    parts = [(2, t) for t in range(tiles)]

    def prepare_part(t):
        at = cols(t)
        held = piece(wide, 2, 2 * pair + core, at)
        across[2, t] = [
            remote(held, held, (ci, 2 * pair_at(d) + side), across_out[d - 1])
            for d in range(1, pairs)
        ]
        over[2, t] = [remote(held, held, twin, over_out[0])]
        for d in range(1, pairs):
            held = piece(wide, 2, 2 * pair_at(pairs - d) + core, at)
            over[2, t].append(remote(held, held, twin, over_out[d]))

    def spread(key):
        for copy in across[key] + over[key][:1]:
            copy.start()

    def spread_own(*keys):
        @pl.when(leads)
        def _():
            for key in keys:
                spread(key)

    def spread_moved(*keys):
        @pl.when(moves)
        def _():
            for key in keys:
                hop[key].wait_recv()
                for part in parts if key == 2 else [key]:
                    spread(part)

    def forward(key):
        for d in range(1, pairs):
            across[key][d - 1].wait_recv()
            over[key][d].start()

    def gathered(key):
        for copy in over[key]:
            copy.wait_recv()

    def cols(t):
        return pl.ds(t * TILE, TILE)

    for m in range(2):
        prepare(m)
    hop[2] = swap(stage.at[2], piece(wide, 2, me), hop_out)
    for t in range(tiles):
        prepare_part(t)
    loads[0].wait()
    lowered(0)
    pl.semaphore_wait(barrier, n - 1 + c - 1 + 1)
    beyond = pl.ds(width - pool_x.shape[1], pool_x.shape[1])
    pool_swap = swap(pool_v.at[mine, beyond], pool_x.at[mine])
    pool_sent, pool_landed = ticket(0), ticket(1)
    pool_out = [
        remote(
            pool_x.at[mine], pool_x.at[mine], (lax.rem(ci + 2 * d, c), me), pool_sent, pool_landed
        )
        for d in range(1, planes)
    ]
    others = pool_x.at[pl.ds(0, (planes - 1) * share)]
    pool_loads[0].wait()
    send(pool_swap, hop[0])
    spread_own(0)
    loads[1].wait()
    lowered(1)
    send(hop[1])
    spread_own(1)
    blanked(0)
    blanked(1)
    loads[2].wait()
    turned(own.at[2], 0)
    lowered(2)
    send(hop[2])
    spread_own(*parts)
    lab_out[0] = jnp.broadcast_to(labs[...], (8, batch))
    lab_out[1] = jnp.broadcast_to(picks[...], (8, batch))

    @pl.when(leads)
    def _():
        lab_in[0] = lab_out[0]

    lab_swap = swap(lab_out, lab_in)
    send(lab_swap)
    lane = lax.broadcasted_iota(jnp.int32, (batch, LANES), 1)
    supply = pool_v.shape[0]
    reach = [(m, min(width, supply - m * width)) for m in range(-(-supply // width))]

    def choose(row_of):
        for k in range(supply // LANES):
            m, at = k * LANES // width, k * LANES % width
            grad[m, 0:batch, at : at + LANES] = (
                (row_of == lane + k * LANES).astype(F32).astype(BF16)
            )

    def picked_of(rs, source, at):
        return sum(
            dot_nn(grad[m, rs, 0:size], source[pl.ds(m * width, size), at]) for m, size in reach
        ).astype(BF16)

    choose(jnp.broadcast_to(picks[...], (LANES, batch)).T)
    for copy in pool_loads[1:]:
        copy.wait()
    direct = width - pool_x.shape[1]
    row_swap, row_sent = [], ticket(0)
    for rs in blocks:
        for k in range(direct // TILE):
            picked = picked_of(rs, pool_v, cols(k))
            rows_out[rs, cols(k)] = picked

            @pl.when(leads)
            def _():
                rows[rs, cols(k)] = picked

        row_swap.append(swap(rows_out.at[rs, 0:direct], rows.at[rs, 0:direct], row_sent))
        send(row_swap[-1])
    @pl.when(leads)
    def _():
        for k in range(direct // TILE, tiles):
            rows[:, cols(k)] = picked_of(everyone, pool_v, cols(k))

    @pl.when(moves)
    def _():
        pool_swap.wait_recv()

        @pl.when(plane < planes // 2)
        def _():
            for copy in pool_out[::-1]:
                copy.start()

        @pl.when(plane >= planes // 2)
        def _():
            for copy in pool_out:
                copy.start()
    spread_moved(0, 1, 2)
    forward(0)
    for copy in loads[3:6]:
        copy.wait()
    turned(edge.at[2], 1)

    def differences(m, at):
        mine = own[m, at, :]
        fixed = edge[m, at, :]
        left = jnp.where(ci == 0, fixed, before[m, at, :].astype(F32))
        right = jnp.where(ci == c - 1, fixed, after[m, at, :].astype(F32))
        return right - mine, mine - left

    zero = jnp.zeros((8, LANES), F32)
    arrive(lab_swap)
    lab_t[...] = jnp.broadcast_to(lab_in[0][0:1, :], (LANES, batch)).T
    @pl.when(moves)
    def _():
        choose(jnp.broadcast_to(lab_in[1][0:1, :], (LANES, batch)).T)
        landed(others, pool_landed)
    @pl.when(moves)
    def _():
        for k in range(direct // TILE, tiles):
            rows[:, cols(k)] = picked_of(everyone, pool_x, cols(k - direct // TILE))
    forward(1)
    gathered(0)

    def activate(rs):
        for t in range(tiles):
            at = cols(t)
            pre = dot_nn(rows[rs, :], wide[0, :, at])
            sig = jax.nn.sigmoid(pre)
            value = (pre * sig).astype(BF16)
            hid[rs, at] = value
            hid_t[at, rs] = value.T
            slope[rs, at] = sig * (1.0 + pre * (1.0 - sig))

    def residual(rs):
        for t in range(tiles):
            at = cols(t)
            value = (rows[rs, at].astype(F32) + dot_nn(hid[rs, :], wide[1, :, at])).astype(BF16)
            resid[rs, at] = value
            resid_t[at, rs] = value.T

    ups = remote(near, before, (lax.rem(ci + 1, c), me))
    downs = remote(near, after, (lax.rem(ci + c - 1, c), me))
    has_next, has_prev = ci < c - 1, ci > 0

    for b, rs in enumerate(blocks):
        if b == len(blocks) - 1:

            @pl.when(moves)
            def _():
                for key in parts[:-1]:
                    forward(key)
        arrive(row_swap[b])
        activate(rs)
        if b == 0:
            @pl.when(leads)
            def _():
                for key in parts:
                    forward(key)
            gathered(1)
            @pl.when(has_next)
            def _():
                ups.start()

            @pl.when(has_prev)
            def _():
                downs.start()

        if b == len(blocks) - 1:

            @pl.when(moves)
            def _():
                forward(parts[-1])
        residual(rs)

    def classify(t, energy):
        at = column(t)
        logits = dot_nn(resid[...], wide[2, :, at])
        out = []
        for k in range(TILE // LANES):
            target = (lab_t[...] == lane + (t * TILE + k * LANES)).astype(F32)
            err = logits[:, k * LANES : (k + 1) * LANES] - target
            energy = energy + fold(err * err)
            out.append((err * norm).astype(BF16))
        dlog[:, at] = jnp.concatenate(out, axis=1)
        return energy

    def product(m, left_t, right, at):
        half = depth // 2

        @pl.loop(0, 2)
        def _(r):
            of = pl.ds(pl.multiple_of(r * half, half), half)
            grad[m, of, at] = dot_nn(left_t[of, :], right[:, at]).astype(BF16)

    to_pair, to_home, core_in, pair_in = {}, {}, {}, {}
    core_sent, home_sent = ticket(0), ticket(0)
    pair_sent = [ticket(0) for _ in range(1, pairs)]

    def scatter(key, m, at):
        core_in[key], pair_in[key] = ticket(1), ticket(1)
        for q in range(pairs):
            remote(
                piece(grad, m, 2 * q + 1 - core, at),
                from_core.at[m, q, :, at],
                twin,
                core_sent,
                core_in[key],
            ).start()
        to_pair[key] = []
        for d in range(1, pairs):
            q = pair_at(d)
            held = piece(grad, m, 2 * q + core, at)
            into = from_pair.at[m, d - 1, :, at]
            to_pair[key].append(
                remote(held, into, (ci, 2 * q + side), pair_sent[d - 1], pair_in[key])
            )
        held = piece(grad, m, 2 * pair + core, at)
        to_home[key] = swap(held, last.at[m, :, at], home_sent)

    def combine(m, into, index, terms, at):
        @pl.loop(0, block // step)
        def _(r):
            off = pl.multiple_of(r * step, step)
            of = pl.ds(pl.multiple_of(index * block + off, step), step)
            total = grad[m, of, at].astype(F32)
            for term in terms:
                total = total + term[pl.ds(off, step), :].astype(F32)
            into[pl.ds(off, step), :] = total.astype(BF16)

    def scatter_on(key, m, at):
        landed(from_core.at[m, :, :, at], core_in[key])
        for d in range(1, pairs):
            q = pair_at(d)
            held = piece(grad, m, 2 * q + core, at)
            combine(m, held, 2 * q + core, [from_core.at[m, q, :, at]], at)
            to_pair[key][d - 1].start()

    def scatter_home(key, m, at):
        if pairs > 1:
            landed(from_pair.at[m, :, :, at], pair_in[key])
        terms = [from_core.at[m, pair, :, at]]
        terms += [from_pair.at[m, d, :, at] for d in range(pairs - 1)]

        @pl.when(leads)
        def _():
            combine(m, last.at[m, :, at], 2 * pair + core, terms, at)

        @pl.when(moves)
        def _():
            combine(m, piece(grad, m, 2 * pair + core, at), 2 * pair + core, terms, at)
            to_home[key].start()

    def moved_on(key, m, at):
        @pl.when(moves)
        def _():
            scatter_on(key, m, at)

    def led_on(key, m, at):
        @pl.when(leads)
        def _():
            scatter_on(key, m, at)

    energy = zero
    for t in range(tiles):
        gathered(parts[t])
        energy = classify(t, energy)
        if t > 0:
            moved_on((2, t - 1), 2, cols(t - 1))
        if t == tiles - 1 and tiles > 1:
            led_on((2, 0), 2, cols(0))
        product(2, resid_t, dlog, cols(t))
        scatter((2, t), 2, cols(t))

    power[0] = energy * (0.5 * norm)
    power_swap = swap(power.at[0], power.at[1])
    send(power_swap)

    for t in range(tiles):
        at = cols(t)
        dres[:, at] = dot_nt(dlog[...], wide[2, at, :]).astype(BF16)
        if t == 0:
            moved_on((2, tiles - 1), 2, cols(tiles - 1))
        if t > 0 or tiles == 1:
            led_on((2, t), 2, at)
        product(1, hid_t, dres, at)
        scatter((1, t), 1, at)
        if t > 0:
            scatter_on((1, t - 1), 1, cols(t - 1))
    @pl.when(has_prev)
    def _():
        ups.wait_recv()

    @pl.when(has_next)
    def _():
        downs.wait_recv()

    def span_sums(m, carry):
        def body(r, carry):
            ahead, behind = differences(m, pl.ds(pl.multiple_of(r * step, step), step))
            return (
                carry[0] + fold(ahead * ahead),
                carry[1] + fold(behind * behind),
                carry[2] + fold(ahead * behind),
            )

        return lax.fori_loop(0, block // step, body, carry)

    carry = (zero, zero, zero)
    for m in range(3):
        carry = span_sums(m, carry)
    for k in range(3):
        sums[me, k] = carry[k]
    sums_sent, sums_landed = ticket(0), ticket(1)
    for d in range(1, n):
        remote(
            sums.at[me], sums.at[me], (ci, lax.rem(me + d, n)), sums_sent, sums_landed
        ).start()
    @pl.loop(0, tiles)
    def _(t):
        at = column(t)
        rows_t[at, :] = rows[:, at].T
    scatter_on((1, tiles - 1), 1, cols(tiles - 1))

    ends = [cols(t) for t in range(tiles - 1)]
    ends += [pl.ds(width - 2 * LANES, LANES), pl.ds(width - LANES, LANES)]
    for t, at in enumerate(ends):
        dlog[:, at] = (dot_nt(dres[...], wide[1, at, :]) * slope[:, at]).astype(BF16)
        product(0, rows_t, dlog, at)
        scatter((0, t), 0, at)
        if t > 0:
            scatter_on((0, t - 1), 0, ends[t - 1])
        if t < tiles:

            @pl.when(moves)
            def _():
                scatter_home((2, t), 2, cols(t))
    scatter_on((0, tiles), 0, ends[tiles])

    @pl.when(leads)
    def _():
        for t in range(tiles):
            scatter_home((2, t), 2, cols(t))

    def finish(key, m, cs, carry):
        arrive(to_home[key])

        def body(r, carry):
            at = pl.ds(pl.multiple_of(r * step, step), step)
            total = last[m, at, cs].astype(F32) * factor[m]
            edge[m, at, cs] = total
            return carry[0] + fold(total * tau[m][at, cs]), carry[1] + fold(total * total)

        return lax.fori_loop(0, block // step, body, carry)

    carry = (zero, zero)
    for t in range(tiles):
        scatter_home((1, t), 1, cols(t))
    landed(sums.at[pl.ds(0, n - 1)], sums_landed)

    def over_dp(ref, k):
        total = ref[0, k]
        for j in range(1, n):
            total = total + ref[j, k]
        return whole(total)

    sq_ahead, sq_behind, mixed = (over_dp(sums, k) for k in range(3))
    len_ahead = jnp.sqrt(sq_ahead + EPS)
    len_behind = jnp.sqrt(sq_behind + EPS)
    raw_sq = (
        sq_ahead / (len_ahead * len_ahead)
        + sq_behind / (len_behind * len_behind)
        + 2.0 * mixed / (len_ahead * len_behind)
    )
    raw_len = jnp.sqrt(raw_sq + EPS)
    spans[ci, 0] = jnp.broadcast_to(len_behind, (8, LANES))
    spans[ci, 1] = jnp.broadcast_to(len_ahead, (8, LANES))
    spans_sent, spans_landed = ticket(0), ticket(1)
    for d in range(1, c):
        remote(
            spans.at[ci], spans.at[ci], (lax.rem(ci + d, c), me), spans_sent, spans_landed
        ).start()
    by_ahead = 1.0 / (len_ahead * raw_len)
    by_behind = 1.0 / (len_behind * raw_len)
    for m in range(3):

        def body(r, _, m=m):
            at = pl.ds(pl.multiple_of(r * step, step), step)
            ahead, behind = differences(m, at)
            tau[m][at, :] = ahead * by_ahead + behind * by_behind
            return 0

        lax.fori_loop(0, block // step, body, 0)

    def flipped(source, cs, store):
        for low in range(0, block, LANES):
            at = pl.ds(low, min(LANES, block - low))
            for k in range(cs.start // LANES, (cs.start + cs.size) // LANES):
                top = min(classes - k * LANES, LANES)
                store(k * LANES, top, at, source[at, k * LANES : (k + 1) * LANES].T)

    def keep_tau(low, top, at, value):
        o_out[0, low : low + top, at] = value[0:top, :]

    def keep_grad(low, top, at, value):
        thin[1, low : low + top, at] = value[0:top, :]

    flipped(tau_out, everything, keep_tau)
    for i in range(tiles):
        carry = finish((2, i), 2, cols(i), carry)
        flipped(edge.at[2], cols(i), keep_grad)
        scatter_home((0, i), 0, ends[i])
    scatter_home((0, tiles), 0, ends[tiles])
    for t in range(tiles):
        carry = finish((1, t), 1, cols(t), carry)
    for t, at in enumerate(ends):
        carry = finish((0, t), 0, at, carry)
    arrive(power_swap)
    late[me, 0] = carry[0]
    late[me, 1] = carry[1]
    late[me, 2] = jnp.where(leads, power[0], power[1])
    late_sent, late_landed = ticket(0), ticket(1)
    for d in range(1, n):
        remote(
            late.at[me], late.at[me], (ci, lax.rem(me + d, n)), late_sent, late_landed
        ).start()
    landed(spans.at[pl.ds(0, c - 1)], spans_landed)
    arc = jnp.zeros((1, 1), F32)
    band = jnp.zeros((1, 1), F32)
    for k in range(c):
        length = spans[k, 0, 0:1, 0:1]
        arc = arc + jnp.where(k <= ci, length, 0.0)
        band = band + length
    band = band + spans[c - 1, 1, 0:1, 0:1]
    landed(late.at[pl.ds(0, n - 1)], late_landed)
    along, g_g, energy_all = (over_dp(late, k) for k in range(3))

    goal = (ci + 1).astype(F32) / (c + 1) * band
    coef = jnp.where(jnp.full((1, 1), climb[0]) == 1, 2.0 * along, along + SPRING * (goal - arc) / band)
    tau_sq = raw_sq / (raw_sq + EPS)
    force_sq = g_g - 2.0 * coef * along + coef * coef * tau_sq
    scale = band / (c + 1) / jnp.sqrt(force_sq + EPS)
    push = scale * coef
    def small(value):
        return jnp.broadcast_to(value, (1, LANES))

    o_small[0:1, :] = small(energy_all)
    o_small[1:2, :] = small(arc / band)
    o_small[2:3, :] = small(0.5 * raw_len)
    for low in range(0, classes, LANES):
        at = pl.ds(low, min(LANES, classes - low))
        o_out[0, at, :] = thin[0, at, :] + (push * o_out[0, at, :] - scale * thin[1, at, :])

    for m in range(2):

        @pl.loop(0, block // step)
        def _(r):
            at = pl.ds(pl.multiple_of(r * step, step), step)
            tau[m][at, :] = own[m, at, :] + (push * tau[m][at, :] - scale * edge[m, at, :])
    @pl.when(has_next)
    def _():
        ups.wait_send()

    @pl.when(has_prev)
    def _():
        downs.wait_send()

    @pl.when(moves)
    def _():
        sent(stage, hop_out)
        sent(rows_out.at[:, 0:direct], row_sent)
        sent(others, pool_sent)
        sent(last, home_sent)
        for copy in (pool_swap, lab_swap, power_swap):
            copy.wait_send()

    for out in across_out + over_out:
        sent(stage, out)
    sent(from_core, core_sent)
    for out in pair_sent:
        sent(last, out)
    sent(sums.at[pl.ds(0, n - 1)], sums_sent)
    sent(spans.at[pl.ds(0, c - 1)], spans_sent)
    sent(late.at[pl.ds(0, n - 1)], late_sent)


def on_device(
    n,
    c,
    images_in,
    images_mid,
    images_out,
    ends_in,
    ends_mid,
    ends_out,
    data_pool,
    batch_rows,
    labels,
    climbing,
):
    block, width = images_in.shape[1], images_in.shape[2]
    classes = images_out.shape[2]
    depth = n * block
    batch = batch_rows.shape[1]
    pairs = n // 2
    sends, receives = semaphores(n, width // TILE, 3)
    vmem = pl.BlockSpec(memory_space=pltpu.VMEM)
    anywhere = pl.BlockSpec(memory_space=pl.ANY)
    scalar = pl.BlockSpec(memory_space=pltpu.SMEM)
    outs = pl.pallas_call(
        functools.partial(kernel, n, c, classes),
        out_shape=(
            pltpu.VMEM(images_in.shape, F32),
            pltpu.VMEM(images_mid.shape, F32),
            pltpu.VMEM((1, classes, block), F32),
            pltpu.VMEM((8, LANES), F32),
        ),
        in_specs=[anywhere] * 7 + [vmem] * 2 + [scalar],
        out_specs=[vmem] * 4,
        scratch_shapes=[
            pltpu.VMEM((3, block, width), F32),
            pltpu.VMEM((3, block, width), F32),
            pltpu.VMEM((2, width, block), F32),
            pltpu.VMEM((block, width), F32),
            pltpu.VMEM((3, depth, width), BF16),
            pltpu.VMEM((3, block, width), BF16),
            pltpu.VMEM((3, block, width), BF16),
            pltpu.VMEM((3, block, width), BF16),
            pltpu.VMEM((3, block, width), BF16),
            pltpu.VMEM(data_pool.shape, BF16),
            pltpu.VMEM((data_pool.shape[0], width // 2), BF16),
            pltpu.VMEM((batch, LANES), jnp.int32),
            pltpu.VMEM((2, 8, batch), jnp.int32),
            pltpu.VMEM((2, 8, batch), jnp.int32),
            pltpu.VMEM((batch, depth), BF16),
            pltpu.VMEM((batch, depth), BF16),
            pltpu.VMEM((batch, width), F32),
            pltpu.VMEM((batch, width), BF16),
            pltpu.VMEM((batch, depth), BF16),
            pltpu.VMEM((depth, batch), BF16),
            pltpu.VMEM((width, batch), BF16),
            pltpu.VMEM((depth, batch), BF16),
            pltpu.VMEM((batch, width), BF16),
            pltpu.VMEM((batch, depth), BF16),
            pltpu.VMEM((3, depth, width), BF16),
            pltpu.VMEM((3, pairs, block, width), BF16),
            pltpu.VMEM((3, max(pairs - 1, 1), block, width), BF16),
            pltpu.VMEM((3, block, width), BF16),
            pltpu.VMEM((2, 8, LANES), F32),
            pltpu.VMEM((n, 3, 8, LANES), F32),
            pltpu.VMEM((c, 2, 8, LANES), F32),
            pltpu.VMEM((n, 3, 8, LANES), F32),
            pltpu.SemaphoreType.DMA((6 + c // 2,)),
            pltpu.SemaphoreType.DMA((sends,)),
            pltpu.SemaphoreType.DMA((receives,)),
        ],
        compiler_params=pltpu.CompilerParams(
            collective_id=0, has_side_effects=True, vmem_limit_bytes=60 * 1024 * 1024
        ),
    )(
        images_in,
        images_mid,
        jnp.swapaxes(images_out, 1, 2),
        ends_in,
        ends_mid,
        jnp.swapaxes(ends_out, 1, 2),
        data_pool,
        batch_rows,
        labels,
        climbing,
    )
    return (outs[0], outs[1], jnp.swapaxes(outs[2], 1, 2), *(outs[3][k, 0:1] for k in range(3)))


def solution(mesh):
    placed = (
        P("chain", "dp", None),
        P("chain", "dp", None),
        P("chain", "dp", None),
        P(None, "dp", None),
        P(None, "dp", None),
        P(None, "dp", None),
        P("dp", None),
        P("chain", "dp"),
        P("chain", "dp"),
        P("chain"),
    )
    return jax.shard_map(
        functools.partial(on_device, mesh.shape["dp"], mesh.shape["chain"]),
        mesh=mesh,
        in_specs=placed,
        out_specs=(
            P("chain", "dp", None),
            P("chain", "dp", None),
            P("chain", "dp", None),
            P("chain"),
            P("chain"),
            P("chain"),
        ),
        check_vma=False,
    )
```

```python
import functools

import jax
import jax.numpy as jnp
from jax import lax
from jax.experimental import pallas as pl
from jax.experimental.pallas import tpu as pltpu
from jax.sharding import PartitionSpec as P

SPRING = 0.03
EPS = 1e-06
TILE = 256
LANES = 128
F32 = jnp.float32
BF16 = jnp.bfloat16


def semaphores(count, chunks, rows):
    pairs = count // 2
    sends = 1 + (pairs - 1) + pairs + 2 + 5 + 3 + 1 + (pairs - 1) + 1 + 1
    receives = (2 + chunks) * ((pairs - 1) + pairs) + 3 + 2 + 4 + rows + 3 + 9 * chunks + 3 + 1
    return sends, receives


def dot_nn(left, right):
    return jnp.dot(left, right, preferred_element_type=F32)


def dot_nt(left, right):
    return lax.dot_general(left, right, (((1,), (1,)), ((), ())), preferred_element_type=F32)


def dot_tn(left, right):
    return lax.dot_general(left, right, (((0,), (0,)), ((), ())), preferred_element_type=F32)


def fold(value):
    part = jnp.sum(value.reshape(value.shape[0] // 8, 8, value.shape[1]), axis=0)
    total = part[:, :LANES]
    for k in range(1, value.shape[1] // LANES):
        total = total + part[:, k * LANES : (k + 1) * LANES]
    return total


def whole(tile):
    return jnp.sum(tile, axis=(0, 1), keepdims=True)


def kernel(
    n,
    c,
    classes,
    p_in,
    p_mid,
    p_out,
    e_in,
    e_mid,
    e_out,
    pool,
    picks_h,
    labs_h,
    climb,
    o_in,
    o_mid,
    o_out,
    o_small,
    own,
    edge,
    thin,
    tau_out,
    wide,
    stage,
    near,
    before,
    after,
    pool_v,
    pool_x,
    both,
    lab_t,
    lab_out,
    lab_in,
    rows_out,
    rows,
    slope,
    hid,
    resid,
    rows_t,
    hid_t,
    resid_t,
    dlog,
    dres,
    grad,
    from_core,
    from_pair,
    last,
    power,
    sums,
    spans,
    late,
    load_sem,
    send_sem,
    recv_sem,
):
    ci, me = lax.axis_index("chain"), lax.axis_index("dp")
    pairs = n // 2
    core, side = lax.rem(ci, 2), lax.rem(me, 2)
    pair = me // 2
    leads = core == side
    moves = core != side
    cross = (ci + 1 - 2 * core, me + 1 - 2 * side)
    twin = (ci + 1 - 2 * core, me)
    block, width = own.shape[1], own.shape[2]
    depth = n * block
    step = min(32, block)
    batch = rows.shape[0]
    tiles = width // TILE
    factor = (depth**-0.5, width**-0.5, depth**-0.5)
    norm = 1.0 / (batch * n * classes)
    counts = [0, 0]
    tau = [o_in.at[0], o_mid.at[0], tau_out]

    def ticket(kind):
        counts[kind] += 1
        return counts[kind] - 1

    def remote(src, dst, to, out=None, into=None):
        return pltpu.make_async_remote_copy(
            src_ref=src,
            dst_ref=dst,
            send_sem=send_sem.at[ticket(0) if out is None else out],
            recv_sem=recv_sem.at[ticket(1) if into is None else into],
            device_id=to,
            device_id_type=pl.DeviceIdType.MESH,
        )

    def sent(ref, out):
        remote(ref, ref, twin, out, 0).wait_send()

    def landed(ref, into):
        remote(ref, ref, twin, 0, into).wait_recv()

    def pair_at(d):
        return lax.rem(pair + d, pairs)
    barrier = pltpu.get_barrier_semaphore()
    for d in range(1, n):
        pl.semaphore_signal(
            barrier, inc=1, device_id=(ci, lax.rem(me + d, n)), device_id_type=pl.DeviceIdType.MESH
        )
    for d in range(1, c):
        pl.semaphore_signal(
            barrier, inc=1, device_id=(lax.rem(ci + d, c), me), device_id_type=pl.DeviceIdType.MESH
        )

    pl.semaphore_signal(barrier, inc=1, device_id=cross, device_id_type=pl.DeviceIdType.MESH)

    end = jnp.where(ci == 0, 0, 1)
    planes, plane = c // 2, ci // 2
    share = pool_v.shape[0] // planes
    mine = pl.ds(pl.multiple_of(plane * share, share), share)

    def load(k, src, dst):
        return pltpu.make_async_copy(src, dst, load_sem.at[k])

    def pool_rows(d):
        return pl.ds(pl.multiple_of(lax.rem(plane + d, planes) * share, share), share)

    loads = [
        load(0, p_in.at[0], own.at[0]),
        load(1, p_mid.at[0], own.at[1]),
        load(2, p_out.at[0], thin.at[0, pl.ds(0, classes)]),
        load(3, e_in.at[end], edge.at[0]),
        load(4, e_mid.at[end], edge.at[1]),
        load(5, e_out.at[end], thin.at[1, pl.ds(0, classes)]),
        load(6, picks_h, both.at[1, 0:1]),
        load(7, labs_h, both.at[0, 0:1]),
    ]
    pool_loads = [
        load(8 + d, pool.at[pool_rows(d)], pool_v.at[pool_rows(d)]) for d in range(planes)
    ]
    for copy in (
        [pool_loads[0], loads[0]] + loads[6:8] + loads[1:3] + pool_loads[1:] + loads[3:6]
    ):
        copy.start()

    def turned(into, thin_at):
        @pl.loop(0, width // LANES)
        def _(k):
            at = pl.ds(pl.multiple_of(k * LANES, LANES), LANES)
            into[:, at] = thin[thin_at, at, :].T

    def blanked(thin_at):
        if classes < width:
            thin[thin_at, pl.ds(classes, width - classes), :] = jnp.zeros(
                (width - classes, block), F32
            )

    def lowered(m):
        def body(r, _):
            off = pl.multiple_of(r * step, step)
            value = own[m, pl.ds(off, step), :]
            low = (value * factor[m]).astype(BF16)
            stage[m, pl.ds(off, step), :] = low

            @pl.when(leads)
            def _():
                wide[m, pl.ds(pl.multiple_of(me * block + off, step), step), :] = low

            near[m, pl.ds(off, step), :] = value.astype(BF16)
            return 0

        lax.fori_loop(0, block // step, body, 0)

    def column(t):
        return pl.ds(pl.multiple_of(t * TILE, TILE), TILE)

    everything, everyone = pl.ds(0, width), pl.ds(0, batch)
    cuts = [0] + [at for at in (batch - 3 * LANES, batch - LANES) if at > 0] + [batch]
    blocks = [pl.ds(low, high - low) for low, high in zip(cuts[:-1], cuts[1:])]

    def piece(ref, m, index, at=everything):
        return ref.at[m, pl.ds(pl.multiple_of(index * block, block), block), at]

    hop, across, over = {}, {}, {}
    def swap(src, dst, out=None):
        return remote(src, dst, cross, out)

    def send(*copies):
        @pl.when(moves)
        def _():
            for copy in copies:
                copy.start()

    def arrive(*copies):
        @pl.when(moves)
        def _():
            for copy in copies:
                copy.wait_recv()

    hop_out = ticket(0)
    across_out = [ticket(0) for _ in range(1, pairs)]
    over_out = [ticket(0) for _ in range(pairs)]

    def prepare(m):
        hop[m] = swap(stage.at[m], piece(wide, m, me), hop_out)
        held = piece(wide, m, 2 * pair + core)
        across[m] = [
            remote(held, held, (ci, 2 * pair_at(d) + side), across_out[d - 1])
            for d in range(1, pairs)
        ]
        over[m] = [remote(held, held, twin, over_out[0])]
        for d in range(1, pairs):
            held = piece(wide, m, 2 * pair_at(pairs - d) + core)
            over[m].append(remote(held, held, twin, over_out[d]))

    parts = [(2, t) for t in range(tiles)]

    def prepare_part(t):
        at = cols(t)
        held = piece(wide, 2, 2 * pair + core, at)
        across[2, t] = [
            remote(held, held, (ci, 2 * pair_at(d) + side), across_out[d - 1])
            for d in range(1, pairs)
        ]
        over[2, t] = [remote(held, held, twin, over_out[0])]
        for d in range(1, pairs):
            held = piece(wide, 2, 2 * pair_at(pairs - d) + core, at)
            over[2, t].append(remote(held, held, twin, over_out[d]))

    def spread(key):
        for copy in across[key] + over[key][:1]:
            copy.start()

    def spread_own(*keys):
        @pl.when(leads)
        def _():
            for key in keys:
                spread(key)

    def spread_moved(*keys):
        @pl.when(moves)
        def _():
            for key in keys:
                hop[key].wait_recv()
                for part in parts if key == 2 else [key]:
                    spread(part)

    def forward(key):
        for d in range(1, pairs):
            across[key][d - 1].wait_recv()
            over[key][d].start()

    def gathered(key):
        for copy in over[key]:
            copy.wait_recv()

    def cols(t):
        return pl.ds(t * TILE, TILE)

    for m in range(2):
        prepare(m)
    hop[2] = swap(stage.at[2], piece(wide, 2, me), hop_out)
    for t in range(tiles):
        prepare_part(t)
    loads[0].wait()
    lowered(0)
    pl.semaphore_wait(barrier, n - 1 + c - 1 + 1)
    beyond = pl.ds(width - pool_x.shape[1], pool_x.shape[1])
    pool_swap = swap(pool_v.at[mine, beyond], pool_x.at[mine])
    pool_sent, pool_landed = ticket(0), ticket(1)
    pool_out = [
        remote(
            pool_x.at[mine], pool_x.at[mine], (lax.rem(ci + 2 * d, c), me), pool_sent, pool_landed
        )
        for d in range(1, planes)
    ]
    others = pool_x.at[pl.ds(0, (planes - 1) * share)]
    pool_loads[0].wait()
    send(pool_swap, hop[0])
    spread_own(0)
    loads[1].wait()
    lowered(1)
    send(hop[1])
    spread_own(1)
    blanked(0)
    blanked(1)
    loads[2].wait()
    turned(own.at[2], 0)
    lowered(2)
    send(hop[2])
    spread_own(*parts)
    loads[6].wait()
    loads[7].wait()
    lab_out[0] = jnp.broadcast_to(both[0][0:1, :], (8, batch))
    lab_out[1] = jnp.broadcast_to(both[1][0:1, :], (8, batch))

    @pl.when(leads)
    def _():
        lab_in[0] = lab_out[0]

    lab_swap = swap(lab_out, lab_in)
    send(lab_swap)
    lane = lax.broadcasted_iota(jnp.int32, (batch, LANES), 1)
    supply = pool_v.shape[0]
    reach = [(m, min(width, supply - m * width)) for m in range(-(-supply // width))]

    def choose(row_of):
        for k in range(supply // LANES):
            m, at = k * LANES // width, k * LANES % width
            grad[m, 0:batch, at : at + LANES] = (
                (row_of == lane + k * LANES).astype(F32).astype(BF16)
            )

    def picked_of(rs, source, at):
        return sum(
            dot_nn(grad[m, rs, 0:size], source[pl.ds(m * width, size), at]) for m, size in reach
        ).astype(BF16)

    choose(jnp.broadcast_to(both[1][0:1, :], (LANES, batch)).T)
    for copy in pool_loads[1:]:
        copy.wait()
    direct = width - pool_x.shape[1]
    row_swap, row_sent = [], ticket(0)
    for rs in blocks:
        for k in range(direct // TILE):
            picked = picked_of(rs, pool_v, cols(k))
            rows_out[rs, cols(k)] = picked

            @pl.when(leads)
            def _():
                rows[rs, cols(k)] = picked

        row_swap.append(swap(rows_out.at[rs, 0:direct], rows.at[rs, 0:direct], row_sent))
        send(row_swap[-1])
    @pl.when(leads)
    def _():
        for k in range(direct // TILE, tiles):
            rows[:, cols(k)] = picked_of(everyone, pool_v, cols(k))

    @pl.when(moves)
    def _():
        pool_swap.wait_recv()

        @pl.when(plane < planes // 2)
        def _():
            for copy in pool_out[::-1]:
                copy.start()

        @pl.when(plane >= planes // 2)
        def _():
            for copy in pool_out:
                copy.start()
    spread_moved(0, 1, 2)
    forward(0)
    for copy in loads[3:6]:
        copy.wait()
    turned(edge.at[2], 1)

    def differences(m, at):
        mine = own[m, at, :]
        fixed = edge[m, at, :]
        left = jnp.where(ci == 0, fixed, before[m, at, :].astype(F32))
        right = jnp.where(ci == c - 1, fixed, after[m, at, :].astype(F32))
        return right - mine, mine - left

    zero = jnp.zeros((8, LANES), F32)
    arrive(lab_swap)
    lab_t[...] = jnp.broadcast_to(lab_in[0][0:1, :], (LANES, batch)).T
    @pl.when(moves)
    def _():
        choose(jnp.broadcast_to(lab_in[1][0:1, :], (LANES, batch)).T)
        landed(others, pool_landed)
    @pl.when(moves)
    def _():
        for k in range(direct // TILE, tiles):
            rows[:, cols(k)] = picked_of(everyone, pool_x, cols(k - direct // TILE))
    forward(1)
    gathered(0)

    def activate(rs):
        for t in range(tiles):
            at = cols(t)
            pre = dot_nn(rows[rs, :], wide[0, :, at])
            sig = jax.nn.sigmoid(pre)
            value = (pre * sig).astype(BF16)
            hid[rs, at] = value
            hid_t[at, rs] = value.T
            slope[rs, at] = sig * (1.0 + pre * (1.0 - sig))

    def residual(rs):
        for t in range(tiles):
            at = cols(t)
            value = (rows[rs, at].astype(F32) + dot_nn(hid[rs, :], wide[1, :, at])).astype(BF16)
            resid[rs, at] = value
            resid_t[at, rs] = value.T

    ups = remote(near, before, (lax.rem(ci + 1, c), me))
    downs = remote(near, after, (lax.rem(ci + c - 1, c), me))
    has_next, has_prev = ci < c - 1, ci > 0

    for b, rs in enumerate(blocks):
        if b == len(blocks) - 1:

            @pl.when(moves)
            def _():
                for key in parts[:-1]:
                    forward(key)
        arrive(row_swap[b])
        activate(rs)
        if b == 0:
            @pl.when(leads)
            def _():
                for key in parts:
                    forward(key)
            gathered(1)
            @pl.when(has_next)
            def _():
                ups.start()

            @pl.when(has_prev)
            def _():
                downs.start()

        if b == len(blocks) - 1:

            @pl.when(moves)
            def _():
                forward(parts[-1])
        residual(rs)

    def classify(t, energy):
        at = column(t)
        logits = dot_nn(resid[...], wide[2, :, at])
        out = []
        for k in range(TILE // LANES):
            target = (lab_t[...] == lane + (t * TILE + k * LANES)).astype(F32)
            err = logits[:, k * LANES : (k + 1) * LANES] - target
            energy = energy + fold(err * err)
            out.append((err * norm).astype(BF16))
        dlog[:, at] = jnp.concatenate(out, axis=1)
        return energy

    def product(m, left_t, right, at):
        half = depth // 2

        @pl.loop(0, 2)
        def _(r):
            of = pl.ds(pl.multiple_of(r * half, half), half)
            grad[m, of, at] = dot_nn(left_t[of, :], right[:, at]).astype(BF16)

    to_pair, to_home, core_in, pair_in = {}, {}, {}, {}
    core_sent, home_sent = ticket(0), ticket(0)
    pair_sent = [ticket(0) for _ in range(1, pairs)]

    def scatter(key, m, at):
        core_in[key], pair_in[key] = ticket(1), ticket(1)
        for q in range(pairs):
            remote(
                piece(grad, m, 2 * q + 1 - core, at),
                from_core.at[m, q, :, at],
                twin,
                core_sent,
                core_in[key],
            ).start()
        to_pair[key] = []
        for d in range(1, pairs):
            q = pair_at(d)
            held = piece(grad, m, 2 * q + core, at)
            into = from_pair.at[m, d - 1, :, at]
            to_pair[key].append(
                remote(held, into, (ci, 2 * q + side), pair_sent[d - 1], pair_in[key])
            )
        held = piece(grad, m, 2 * pair + core, at)
        to_home[key] = swap(held, last.at[m, :, at], home_sent)

    def combine(m, into, index, terms, at):
        @pl.loop(0, block // step)
        def _(r):
            off = pl.multiple_of(r * step, step)
            of = pl.ds(pl.multiple_of(index * block + off, step), step)
            total = grad[m, of, at].astype(F32)
            for term in terms:
                total = total + term[pl.ds(off, step), :].astype(F32)
            into[pl.ds(off, step), :] = total.astype(BF16)

    def scatter_on(key, m, at):
        landed(from_core.at[m, :, :, at], core_in[key])
        for d in range(1, pairs):
            q = pair_at(d)
            held = piece(grad, m, 2 * q + core, at)
            combine(m, held, 2 * q + core, [from_core.at[m, q, :, at]], at)
            to_pair[key][d - 1].start()

    def scatter_home(key, m, at):
        if pairs > 1:
            landed(from_pair.at[m, :, :, at], pair_in[key])
        terms = [from_core.at[m, pair, :, at]]
        terms += [from_pair.at[m, d, :, at] for d in range(pairs - 1)]

        @pl.when(leads)
        def _():
            combine(m, last.at[m, :, at], 2 * pair + core, terms, at)

        @pl.when(moves)
        def _():
            combine(m, piece(grad, m, 2 * pair + core, at), 2 * pair + core, terms, at)
            to_home[key].start()

    def moved_on(key, m, at):
        @pl.when(moves)
        def _():
            scatter_on(key, m, at)

    def led_on(key, m, at):
        @pl.when(leads)
        def _():
            scatter_on(key, m, at)

    energy = zero
    for t in range(tiles):
        gathered(parts[t])
        energy = classify(t, energy)
        if t > 0:
            moved_on((2, t - 1), 2, cols(t - 1))
        if t == tiles - 1 and tiles > 1:
            led_on((2, 0), 2, cols(0))
        product(2, resid_t, dlog, cols(t))
        scatter((2, t), 2, cols(t))

    power[0] = energy * (0.5 * norm)
    power_swap = swap(power.at[0], power.at[1])
    send(power_swap)

    for t in range(tiles):
        at = cols(t)
        dres[:, at] = dot_nt(dlog[...], wide[2, at, :]).astype(BF16)
        if t == 0:
            moved_on((2, tiles - 1), 2, cols(tiles - 1))
        if t > 0 or tiles == 1:
            led_on((2, t), 2, at)
        product(1, hid_t, dres, at)
        scatter((1, t), 1, at)
        if t > 0:
            scatter_on((1, t - 1), 1, cols(t - 1))
    @pl.when(has_prev)
    def _():
        ups.wait_recv()

    @pl.when(has_next)
    def _():
        downs.wait_recv()

    def span_sums(m, carry):
        def body(r, carry):
            ahead, behind = differences(m, pl.ds(pl.multiple_of(r * step, step), step))
            return (
                carry[0] + fold(ahead * ahead),
                carry[1] + fold(behind * behind),
                carry[2] + fold(ahead * behind),
            )

        return lax.fori_loop(0, block // step, body, carry)

    carry = (zero, zero, zero)
    for m in range(3):
        carry = span_sums(m, carry)
    for k in range(3):
        sums[me, k] = carry[k]
    sums_sent, sums_landed = ticket(0), ticket(1)
    for d in range(1, n):
        remote(
            sums.at[me], sums.at[me], (ci, lax.rem(me + d, n)), sums_sent, sums_landed
        ).start()
    @pl.loop(0, tiles)
    def _(t):
        at = column(t)
        rows_t[at, :] = rows[:, at].T
    scatter_on((1, tiles - 1), 1, cols(tiles - 1))

    ends = [cols(t) for t in range(tiles - 1)]
    ends += [pl.ds(width - 2 * LANES, LANES), pl.ds(width - LANES, LANES)]
    for t, at in enumerate(ends):
        dlog[:, at] = (dot_nt(dres[...], wide[1, at, :]) * slope[:, at]).astype(BF16)
        product(0, rows_t, dlog, at)
        scatter((0, t), 0, at)
        if t > 0:
            moved_on((0, t - 1), 0, ends[t - 1])
        if t < tiles:

            @pl.when(moves)
            def _():
                scatter_home((2, t), 2, cols(t))
    moved_on((0, tiles), 0, ends[tiles])

    @pl.when(leads)
    def _():
        for t in range(tiles):
            scatter_home((2, t), 2, cols(t))

    def finish(key, m, cs, carry):
        arrive(to_home[key])

        def body(r, carry):
            at = pl.ds(pl.multiple_of(r * step, step), step)
            total = last[m, at, cs].astype(F32) * factor[m]
            edge[m, at, cs] = total
            return carry[0] + fold(total * tau[m][at, cs]), carry[1] + fold(total * total)

        return lax.fori_loop(0, block // step, body, carry)

    carry = (zero, zero)
    for t in range(tiles):
        scatter_home((1, t), 1, cols(t))
        if t == tiles // 2:
            for k, at in enumerate(ends):
                led_on((0, k), 0, at)
    landed(sums.at[pl.ds(0, n - 1)], sums_landed)

    def over_dp(ref, k):
        total = ref[0, k]
        for j in range(1, n):
            total = total + ref[j, k]
        return whole(total)

    sq_ahead, sq_behind, mixed = (over_dp(sums, k) for k in range(3))
    len_ahead = jnp.sqrt(sq_ahead + EPS)
    len_behind = jnp.sqrt(sq_behind + EPS)
    raw_sq = (
        sq_ahead / (len_ahead * len_ahead)
        + sq_behind / (len_behind * len_behind)
        + 2.0 * mixed / (len_ahead * len_behind)
    )
    raw_len = jnp.sqrt(raw_sq + EPS)
    spans[ci, 0] = jnp.broadcast_to(len_behind, (8, LANES))
    spans[ci, 1] = jnp.broadcast_to(len_ahead, (8, LANES))
    spans_sent, spans_landed = ticket(0), ticket(1)
    for d in range(1, c):
        remote(
            spans.at[ci], spans.at[ci], (lax.rem(ci + d, c), me), spans_sent, spans_landed
        ).start()
    by_ahead = 1.0 / (len_ahead * raw_len)
    by_behind = 1.0 / (len_behind * raw_len)
    for m in range(3):

        def body(r, _, m=m):
            at = pl.ds(pl.multiple_of(r * step, step), step)
            ahead, behind = differences(m, at)
            tau[m][at, :] = ahead * by_ahead + behind * by_behind
            return 0

        lax.fori_loop(0, block // step, body, 0)

    def flipped(source, cs, store):
        for low in range(0, block, LANES):
            at = pl.ds(low, min(LANES, block - low))
            for k in range(cs.start // LANES, (cs.start + cs.size) // LANES):
                top = min(classes - k * LANES, LANES)
                store(k * LANES, top, at, source[at, k * LANES : (k + 1) * LANES].T)

    def keep_tau(low, top, at, value):
        o_out[0, low : low + top, at] = value[0:top, :]

    def keep_grad(low, top, at, value):
        thin[1, low : low + top, at] = value[0:top, :]

    flipped(tau_out, everything, keep_tau)
    for i in range(tiles):
        carry = finish((2, i), 2, cols(i), carry)
        flipped(edge.at[2], cols(i), keep_grad)
        scatter_home((0, i), 0, ends[i])
    for t in range(tiles):
        carry = finish((1, t), 1, cols(t), carry)
    scatter_home((0, tiles), 0, ends[tiles])
    for t, at in enumerate(ends):
        carry = finish((0, t), 0, at, carry)
    arrive(power_swap)
    terms = (carry[0], carry[1], jnp.where(leads, power[0], power[1]))
    for k, term in enumerate(terms):
        late[me, k : k + 1, :] = jnp.sum(term, axis=0, keepdims=True)
    late[me, 3:8, :] = jnp.zeros((5, LANES), F32)
    late_sent, late_landed = ticket(0), ticket(1)
    for d in range(1, n):
        remote(
            late.at[me], late.at[me], (ci, lax.rem(me + d, n)), late_sent, late_landed
        ).start()
    landed(spans.at[pl.ds(0, c - 1)], spans_landed)
    arc = jnp.zeros((1, 1), F32)
    band = jnp.zeros((1, 1), F32)
    for k in range(c):
        length = spans[k, 0, 0:1, 0:1]
        arc = arc + jnp.where(k <= ci, length, 0.0)
        band = band + length
    band = band + spans[c - 1, 1, 0:1, 0:1]
    landed(late.at[pl.ds(0, n - 1)], late_landed)
    closing = late[0]
    for j in range(1, n):
        closing = closing + late[j]
    closing = jnp.sum(closing, axis=1, keepdims=True)
    along, g_g, energy_all = closing[0:1], closing[1:2], closing[2:3]

    goal = (ci + 1).astype(F32) / (c + 1) * band
    coef = jnp.where(jnp.full((1, 1), climb[0]) == 1, 2.0 * along, along + SPRING * (goal - arc) / band)
    tau_sq = raw_sq / (raw_sq + EPS)
    force_sq = g_g - 2.0 * coef * along + coef * coef * tau_sq
    scale = band / (c + 1) / jnp.sqrt(force_sq + EPS)
    push = scale * coef
    def small(value):
        return jnp.broadcast_to(value, (1, LANES))

    o_small[0:1, :] = small(energy_all)
    o_small[1:2, :] = small(arc / band)
    o_small[2:3, :] = small(0.5 * raw_len)
    for low in range(0, classes, LANES):
        at = pl.ds(low, min(LANES, classes - low))
        o_out[0, at, :] = thin[0, at, :] + (push * o_out[0, at, :] - scale * thin[1, at, :])

    for m in range(2):

        @pl.loop(0, block // step)
        def _(r):
            at = pl.ds(pl.multiple_of(r * step, step), step)
            tau[m][at, :] = own[m, at, :] + (push * tau[m][at, :] - scale * edge[m, at, :])
    @pl.when(has_next)
    def _():
        ups.wait_send()

    @pl.when(has_prev)
    def _():
        downs.wait_send()

    @pl.when(moves)
    def _():
        sent(stage, hop_out)
        sent(rows_out.at[:, 0:direct], row_sent)
        sent(others, pool_sent)
        sent(last, home_sent)
        for copy in (pool_swap, lab_swap, power_swap):
            copy.wait_send()

    for out in across_out + over_out:
        sent(stage, out)
    sent(from_core, core_sent)
    for out in pair_sent:
        sent(last, out)
    sent(sums.at[pl.ds(0, n - 1)], sums_sent)
    sent(spans.at[pl.ds(0, c - 1)], spans_sent)
    sent(late.at[pl.ds(0, n - 1)], late_sent)


def on_device(
    n,
    c,
    images_in,
    images_mid,
    images_out,
    ends_in,
    ends_mid,
    ends_out,
    data_pool,
    batch_rows,
    labels,
    climbing,
):
    block, width = images_in.shape[1], images_in.shape[2]
    classes = images_out.shape[2]
    depth = n * block
    batch = batch_rows.shape[1]
    pairs = n // 2
    sends, receives = semaphores(n, width // TILE, 3)
    vmem = pl.BlockSpec(memory_space=pltpu.VMEM)
    anywhere = pl.BlockSpec(memory_space=pl.ANY)
    scalar = pl.BlockSpec(memory_space=pltpu.SMEM)
    outs = pl.pallas_call(
        functools.partial(kernel, n, c, classes),
        out_shape=(
            pltpu.VMEM(images_in.shape, F32),
            pltpu.VMEM(images_mid.shape, F32),
            pltpu.VMEM((1, classes, block), F32),
            pltpu.VMEM((8, LANES), F32),
        ),
        in_specs=[anywhere] * 9 + [scalar],
        out_specs=[vmem] * 4,
        scratch_shapes=[
            pltpu.VMEM((3, block, width), F32),
            pltpu.VMEM((3, block, width), F32),
            pltpu.VMEM((2, width, block), F32),
            pltpu.VMEM((block, width), F32),
            pltpu.VMEM((3, depth, width), BF16),
            pltpu.VMEM((3, block, width), BF16),
            pltpu.VMEM((3, block, width), BF16),
            pltpu.VMEM((3, block, width), BF16),
            pltpu.VMEM((3, block, width), BF16),
            pltpu.VMEM(data_pool.shape, BF16),
            pltpu.VMEM((data_pool.shape[0], width // 2), BF16),
            pltpu.VMEM((2, 8, batch), jnp.int32),
            pltpu.VMEM((batch, LANES), jnp.int32),
            pltpu.VMEM((2, 8, batch), jnp.int32),
            pltpu.VMEM((2, 8, batch), jnp.int32),
            pltpu.VMEM((batch, depth), BF16),
            pltpu.VMEM((batch, depth), BF16),
            pltpu.VMEM((batch, width), F32),
            pltpu.VMEM((batch, width), BF16),
            pltpu.VMEM((batch, depth), BF16),
            pltpu.VMEM((depth, batch), BF16),
            pltpu.VMEM((width, batch), BF16),
            pltpu.VMEM((depth, batch), BF16),
            pltpu.VMEM((batch, width), BF16),
            pltpu.VMEM((batch, depth), BF16),
            pltpu.VMEM((3, depth, width), BF16),
            pltpu.VMEM((3, pairs, block, width), BF16),
            pltpu.VMEM((3, max(pairs - 1, 1), block, width), BF16),
            pltpu.VMEM((3, block, width), BF16),
            pltpu.VMEM((2, 8, LANES), F32),
            pltpu.VMEM((n, 3, 8, LANES), F32),
            pltpu.VMEM((c, 2, 8, LANES), F32),
            pltpu.VMEM((n, 8, LANES), F32),
            pltpu.SemaphoreType.DMA((8 + c // 2,)),
            pltpu.SemaphoreType.DMA((sends,)),
            pltpu.SemaphoreType.DMA((receives,)),
        ],
        compiler_params=pltpu.CompilerParams(
            collective_id=0, has_side_effects=True, vmem_limit_bytes=60 * 1024 * 1024
        ),
    )(
        images_in,
        images_mid,
        jnp.swapaxes(images_out, 1, 2),
        ends_in,
        ends_mid,
        jnp.swapaxes(ends_out, 1, 2),
        data_pool,
        batch_rows,
        labels,
        climbing,
    )
    return (outs[0], outs[1], jnp.swapaxes(outs[2], 1, 2), *(outs[3][k, 0:1] for k in range(3)))


def solution(mesh):
    placed = (
        P("chain", "dp", None),
        P("chain", "dp", None),
        P("chain", "dp", None),
        P(None, "dp", None),
        P(None, "dp", None),
        P(None, "dp", None),
        P("dp", None),
        P("chain", "dp"),
        P("chain", "dp"),
        P("chain"),
    )
    return jax.shard_map(
        functools.partial(on_device, mesh.shape["dp"], mesh.shape["chain"]),
        mesh=mesh,
        in_specs=placed,
        out_specs=(
            P("chain", "dp", None),
            P("chain", "dp", None),
            P("chain", "dp", None),
            P("chain"),
            P("chain"),
            P("chain"),
        ),
        check_vma=False,
    )
```

```python
import functools

import jax
import jax.numpy as jnp
from jax import lax
from jax.experimental import pallas as pl
from jax.experimental.pallas import tpu as pltpu
from jax.sharding import PartitionSpec as P

SPRING = 0.03
EPS = 1e-06
TILE = 256
LANES = 128
F32 = jnp.float32
BF16 = jnp.bfloat16


def semaphores(count, chunks, rows):
    pairs = count // 2
    sends = 1 + (pairs - 1) + pairs + 2 + 5 + 3 + 1 + (pairs - 1) + 1 + 1
    receives = (2 + chunks) * ((pairs - 1) + pairs) + 3 + 2 + 4 + rows + 3 + 9 * chunks + 3 + 1
    return sends, receives


def dot_nn(left, right):
    return jnp.dot(left, right, preferred_element_type=F32)


def dot_nt(left, right):
    return lax.dot_general(left, right, (((1,), (1,)), ((), ())), preferred_element_type=F32)


def dot_tn(left, right):
    return lax.dot_general(left, right, (((0,), (0,)), ((), ())), preferred_element_type=F32)


def fold(value):
    part = jnp.sum(value.reshape(value.shape[0] // 8, 8, value.shape[1]), axis=0)
    total = part[:, :LANES]
    for k in range(1, value.shape[1] // LANES):
        total = total + part[:, k * LANES : (k + 1) * LANES]
    return total


def whole(tile):
    return jnp.sum(tile, axis=(0, 1), keepdims=True)


def kernel(
    n,
    c,
    classes,
    p_in,
    p_mid,
    p_out,
    e_in,
    e_mid,
    e_out,
    pool,
    picks_h,
    labs_h,
    climb,
    o_in,
    o_mid,
    o_out,
    o_small,
    own,
    edge,
    thin,
    tau_out,
    wide,
    stage,
    near,
    before,
    after,
    pool_v,
    pool_x,
    both,
    lab_t,
    lab_out,
    lab_in,
    rows_out,
    rows,
    slope,
    hid,
    resid,
    rows_t,
    hid_t,
    resid_t,
    dlog,
    dres,
    grad,
    from_core,
    from_pair,
    last,
    power,
    sums,
    spans,
    late,
    load_sem,
    send_sem,
    recv_sem,
):
    ci, me = lax.axis_index("chain"), lax.axis_index("dp")
    pairs = n // 2
    core, side = lax.rem(ci, 2), lax.rem(me, 2)
    pair = me // 2
    leads = core == side
    moves = core != side
    cross = (ci + 1 - 2 * core, me + 1 - 2 * side)
    twin = (ci + 1 - 2 * core, me)
    block, width = own.shape[1], own.shape[2]
    depth = n * block
    step = min(32, block)
    batch = rows.shape[0]
    tiles = width // TILE
    factor = (depth**-0.5, width**-0.5, depth**-0.5)
    norm = 1.0 / (batch * n * classes)
    counts = [0, 0]
    tau = [o_in.at[0], o_mid.at[0], tau_out]

    def ticket(kind):
        counts[kind] += 1
        return counts[kind] - 1

    def remote(src, dst, to, out=None, into=None):
        return pltpu.make_async_remote_copy(
            src_ref=src,
            dst_ref=dst,
            send_sem=send_sem.at[ticket(0) if out is None else out],
            recv_sem=recv_sem.at[ticket(1) if into is None else into],
            device_id=to,
            device_id_type=pl.DeviceIdType.MESH,
        )

    def sent(ref, out):
        remote(ref, ref, twin, out, 0).wait_send()

    def landed(ref, into):
        remote(ref, ref, twin, 0, into).wait_recv()

    def pair_at(d):
        return lax.rem(pair + d, pairs)
    barrier = pltpu.get_barrier_semaphore()
    for d in range(1, n):
        pl.semaphore_signal(
            barrier, inc=1, device_id=(ci, lax.rem(me + d, n)), device_id_type=pl.DeviceIdType.MESH
        )
    for d in range(1, c):
        pl.semaphore_signal(
            barrier, inc=1, device_id=(lax.rem(ci + d, c), me), device_id_type=pl.DeviceIdType.MESH
        )

    pl.semaphore_signal(barrier, inc=1, device_id=cross, device_id_type=pl.DeviceIdType.MESH)

    end = jnp.where(ci == 0, 0, 1)
    planes, plane = c // 2, ci // 2
    share = pool_v.shape[0] // planes
    mine = pl.ds(pl.multiple_of(plane * share, share), share)

    def load(k, src, dst):
        return pltpu.make_async_copy(src, dst, load_sem.at[k])

    def pool_rows(d):
        return pl.ds(pl.multiple_of(lax.rem(plane + d, planes) * share, share), share)

    loads = [
        load(0, p_in.at[0], own.at[0]),
        load(1, p_mid.at[0], own.at[1]),
        load(2, p_out.at[0], thin.at[0, pl.ds(0, classes)]),
        load(3, e_in.at[end], edge.at[0]),
        load(4, e_mid.at[end], edge.at[1]),
        load(5, e_out.at[end], thin.at[1, pl.ds(0, classes)]),
        load(6, picks_h, both.at[1, 0:1]),
        load(7, labs_h, both.at[0, 0:1]),
    ]
    pool_loads = [
        load(8 + d, pool.at[pool_rows(d)], pool_v.at[pool_rows(d)]) for d in range(planes)
    ]
    for copy in (
        [pool_loads[0], loads[0]] + loads[6:8] + loads[1:3] + pool_loads[1:] + loads[3:6]
    ):
        copy.start()

    def turned(into, thin_at):
        @pl.loop(0, width // LANES)
        def _(k):
            at = pl.ds(pl.multiple_of(k * LANES, LANES), LANES)
            into[:, at] = thin[thin_at, at, :].T

    def blanked(thin_at):
        if classes < width:
            thin[thin_at, pl.ds(classes, width - classes), :] = jnp.zeros(
                (width - classes, block), F32
            )

    def lowered(m):
        def body(r, _):
            off = pl.multiple_of(r * step, step)
            value = own[m, pl.ds(off, step), :]
            low = (value * factor[m]).astype(BF16)
            stage[m, pl.ds(off, step), :] = low

            @pl.when(leads)
            def _():
                wide[m, pl.ds(pl.multiple_of(me * block + off, step), step), :] = low

            near[m, pl.ds(off, step), :] = value.astype(BF16)
            return 0

        lax.fori_loop(0, block // step, body, 0)

    def column(t):
        return pl.ds(pl.multiple_of(t * TILE, TILE), TILE)

    everything, everyone = pl.ds(0, width), pl.ds(0, batch)
    cuts = [0] + [at for at in (batch - 3 * LANES, batch - LANES) if at > 0] + [batch]
    blocks = [pl.ds(low, high - low) for low, high in zip(cuts[:-1], cuts[1:])]

    def piece(ref, m, index, at=everything):
        return ref.at[m, pl.ds(pl.multiple_of(index * block, block), block), at]

    hop, across, over = {}, {}, {}
    def swap(src, dst, out=None):
        return remote(src, dst, cross, out)

    def send(*copies):
        @pl.when(moves)
        def _():
            for copy in copies:
                copy.start()

    def arrive(*copies):
        @pl.when(moves)
        def _():
            for copy in copies:
                copy.wait_recv()

    hop_out = ticket(0)
    across_out = [ticket(0) for _ in range(1, pairs)]
    over_out = [ticket(0) for _ in range(pairs)]

    def prepare(m):
        hop[m] = swap(stage.at[m], piece(wide, m, me), hop_out)
        held = piece(wide, m, 2 * pair + core)
        across[m] = [
            remote(held, held, (ci, 2 * pair_at(d) + side), across_out[d - 1])
            for d in range(1, pairs)
        ]
        over[m] = [remote(held, held, twin, over_out[0])]
        for d in range(1, pairs):
            held = piece(wide, m, 2 * pair_at(pairs - d) + core)
            over[m].append(remote(held, held, twin, over_out[d]))

    parts = [(2, t) for t in range(tiles)]

    def prepare_part(t):
        at = cols(t)
        held = piece(wide, 2, 2 * pair + core, at)
        across[2, t] = [
            remote(held, held, (ci, 2 * pair_at(d) + side), across_out[d - 1])
            for d in range(1, pairs)
        ]
        over[2, t] = [remote(held, held, twin, over_out[0])]
        for d in range(1, pairs):
            held = piece(wide, 2, 2 * pair_at(pairs - d) + core, at)
            over[2, t].append(remote(held, held, twin, over_out[d]))

    def spread(key):
        for copy in across[key] + over[key][:1]:
            copy.start()

    def spread_own(*keys):
        @pl.when(leads)
        def _():
            for key in keys:
                spread(key)

    def spread_moved(*keys):
        @pl.when(moves)
        def _():
            for key in keys:
                hop[key].wait_recv()
                for part in parts if key == 2 else [key]:
                    spread(part)

    def forward(key):
        for d in range(1, pairs):
            across[key][d - 1].wait_recv()
            over[key][d].start()

    def gathered(key):
        for copy in over[key]:
            copy.wait_recv()

    def cols(t):
        return pl.ds(t * TILE, TILE)

    for m in range(2):
        prepare(m)
    hop[2] = swap(stage.at[2], piece(wide, 2, me), hop_out)
    for t in range(tiles):
        prepare_part(t)
    loads[0].wait()
    lowered(0)
    pl.semaphore_wait(barrier, n - 1 + c - 1 + 1)
    beyond = pl.ds(width - pool_x.shape[1], pool_x.shape[1])
    pool_swap = swap(pool_v.at[mine, beyond], pool_x.at[mine])
    pool_sent, pool_landed = ticket(0), ticket(1)
    pool_out = [
        remote(
            pool_x.at[mine], pool_x.at[mine], (lax.rem(ci + 2 * d, c), me), pool_sent, pool_landed
        )
        for d in range(1, planes)
    ]
    others = pool_x.at[pl.ds(0, (planes - 1) * share)]
    pool_loads[0].wait()
    send(pool_swap, hop[0])
    spread_own(0)
    loads[1].wait()
    lowered(1)
    send(hop[1])
    spread_own(1)
    blanked(0)
    blanked(1)
    loads[2].wait()
    turned(own.at[2], 0)
    lowered(2)
    send(hop[2])
    spread_own(*parts)
    loads[6].wait()
    loads[7].wait()
    lab_out[0] = jnp.broadcast_to(both[0][0:1, :], (8, batch))
    lab_out[1] = jnp.broadcast_to(both[1][0:1, :], (8, batch))

    @pl.when(leads)
    def _():
        lab_in[0] = lab_out[0]

    lab_swap = swap(lab_out, lab_in)
    send(lab_swap)
    lane = lax.broadcasted_iota(jnp.int32, (batch, LANES), 1)
    supply = pool_v.shape[0]
    reach = [(m, min(width, supply - m * width)) for m in range(-(-supply // width))]

    def choose(row_of):
        for k in range(supply // LANES):
            m, at = k * LANES // width, k * LANES % width
            grad[m, 0:batch, at : at + LANES] = (
                (row_of == lane + k * LANES).astype(F32).astype(BF16)
            )

    def picked_of(rs, source, at):
        return sum(
            dot_nn(grad[m, rs, 0:size], source[pl.ds(m * width, size), at]) for m, size in reach
        ).astype(BF16)

    choose(jnp.broadcast_to(both[1][0:1, :], (LANES, batch)).T)
    for copy in pool_loads[1:]:
        copy.wait()
    direct = width - pool_x.shape[1]
    row_swap, row_sent = [], ticket(0)
    for rs in blocks:
        for k in range(direct // TILE):
            picked = picked_of(rs, pool_v, cols(k))
            rows_out[rs, cols(k)] = picked

            @pl.when(leads)
            def _():
                rows[rs, cols(k)] = picked

        row_swap.append(swap(rows_out.at[rs, 0:direct], rows.at[rs, 0:direct], row_sent))
        send(row_swap[-1])
    @pl.when(leads)
    def _():
        for k in range(direct // TILE, tiles):
            rows[:, cols(k)] = picked_of(everyone, pool_v, cols(k))

    @pl.when(moves)
    def _():
        pool_swap.wait_recv()

        @pl.when(plane < planes // 2)
        def _():
            for copy in pool_out[::-1]:
                copy.start()

        @pl.when(plane >= planes // 2)
        def _():
            for copy in pool_out:
                copy.start()
    spread_moved(0, 1, 2)
    forward(0)
    for copy in loads[3:6]:
        copy.wait()
    turned(edge.at[2], 1)

    def differences(m, at):
        mine = own[m, at, :]
        fixed = edge[m, at, :]
        left = jnp.where(ci == 0, fixed, before[m, at, :].astype(F32))
        right = jnp.where(ci == c - 1, fixed, after[m, at, :].astype(F32))
        return right - mine, mine - left

    zero = jnp.zeros((8, LANES), F32)
    arrive(lab_swap)
    lab_t[...] = jnp.broadcast_to(lab_in[0][0:1, :], (LANES, batch)).T
    @pl.when(moves)
    def _():
        choose(jnp.broadcast_to(lab_in[1][0:1, :], (LANES, batch)).T)
        landed(others, pool_landed)
    @pl.when(moves)
    def _():
        for k in range(direct // TILE, tiles):
            rows[:, cols(k)] = picked_of(everyone, pool_x, cols(k - direct // TILE))
    forward(1)
    gathered(0)

    def activate(rs):
        for t in range(tiles):
            at = cols(t)
            pre = dot_nn(rows[rs, :], wide[0, :, at])
            sig = jax.nn.sigmoid(pre)
            value = (pre * sig).astype(BF16)
            hid[rs, at] = value
            hid_t[at, rs] = value.T
            slope[rs, at] = sig * (1.0 + pre * (1.0 - sig))

    def residual(rs):
        for t in range(tiles):
            at = cols(t)
            value = (rows[rs, at].astype(F32) + dot_nn(hid[rs, :], wide[1, :, at])).astype(BF16)
            resid[rs, at] = value
            resid_t[at, rs] = value.T

    ups = remote(near, before, (lax.rem(ci + 1, c), me))
    downs = remote(near, after, (lax.rem(ci + c - 1, c), me))
    has_next, has_prev = ci < c - 1, ci > 0

    for b, rs in enumerate(blocks):
        if b == len(blocks) - 1:

            @pl.when(moves)
            def _():
                for key in parts[:-1]:
                    forward(key)
        arrive(row_swap[b])
        activate(rs)
        if b == 0:
            @pl.when(leads)
            def _():
                for key in parts:
                    forward(key)
            gathered(1)
            @pl.when(has_next)
            def _():
                ups.start()

            @pl.when(has_prev)
            def _():
                downs.start()

        if b == len(blocks) - 1:

            @pl.when(moves)
            def _():
                forward(parts[-1])
        residual(rs)

    def classify(t, energy):
        at = column(t)
        logits = dot_nn(resid[...], wide[2, :, at])
        out = []
        for k in range(TILE // LANES):
            target = (lab_t[...] == lane + (t * TILE + k * LANES)).astype(F32)
            err = logits[:, k * LANES : (k + 1) * LANES] - target
            energy = energy + fold(err * err)
            out.append((err * norm).astype(BF16))
        dlog[:, at] = jnp.concatenate(out, axis=1)
        return energy

    def product(m, left_t, right, at):
        half = depth // 2

        @pl.loop(0, 2)
        def _(r):
            of = pl.ds(pl.multiple_of(r * half, half), half)
            grad[m, of, at] = dot_nn(left_t[of, :], right[:, at]).astype(BF16)

    to_pair, to_home, core_in, pair_in = {}, {}, {}, {}
    core_sent, home_sent = ticket(0), ticket(0)
    pair_sent = [ticket(0) for _ in range(1, pairs)]

    def scatter(key, m, at):
        core_in[key], pair_in[key] = ticket(1), ticket(1)
        for q in range(pairs):
            remote(
                piece(grad, m, 2 * q + 1 - core, at),
                from_core.at[m, q, :, at],
                twin,
                core_sent,
                core_in[key],
            ).start()
        to_pair[key] = []
        for d in range(1, pairs):
            q = pair_at(d)
            held = piece(grad, m, 2 * q + core, at)
            into = from_pair.at[m, d - 1, :, at]
            to_pair[key].append(
                remote(held, into, (ci, 2 * q + side), pair_sent[d - 1], pair_in[key])
            )
        held = piece(grad, m, 2 * pair + core, at)
        to_home[key] = swap(held, last.at[m, :, at], home_sent)

    def combine(m, into, index, terms, at):
        @pl.loop(0, block // step)
        def _(r):
            off = pl.multiple_of(r * step, step)
            of = pl.ds(pl.multiple_of(index * block + off, step), step)
            total = grad[m, of, at].astype(F32)
            for term in terms:
                total = total + term[pl.ds(off, step), :].astype(F32)
            into[pl.ds(off, step), :] = total.astype(BF16)

    def scatter_on(key, m, at):
        landed(from_core.at[m, :, :, at], core_in[key])
        for d in range(1, pairs):
            q = pair_at(d)
            held = piece(grad, m, 2 * q + core, at)
            combine(m, held, 2 * q + core, [from_core.at[m, q, :, at]], at)
            to_pair[key][d - 1].start()

    def scatter_home(key, m, at):
        if pairs > 1:
            landed(from_pair.at[m, :, :, at], pair_in[key])
        terms = [from_core.at[m, pair, :, at]]
        terms += [from_pair.at[m, d, :, at] for d in range(pairs - 1)]

        @pl.when(leads)
        def _():
            combine(m, last.at[m, :, at], 2 * pair + core, terms, at)

        @pl.when(moves)
        def _():
            combine(m, piece(grad, m, 2 * pair + core, at), 2 * pair + core, terms, at)
            to_home[key].start()

    def moved_on(key, m, at):
        @pl.when(moves)
        def _():
            scatter_on(key, m, at)

    def led_on(key, m, at):
        @pl.when(leads)
        def _():
            scatter_on(key, m, at)

    energy = zero
    for t in range(tiles):
        gathered(parts[t])
        energy = classify(t, energy)
        if t > 0:
            moved_on((2, t - 1), 2, cols(t - 1))
        if t == tiles - 1 and tiles > 1:
            led_on((2, 0), 2, cols(0))
        product(2, resid_t, dlog, cols(t))
        scatter((2, t), 2, cols(t))

    power[0] = energy * (0.5 * norm)
    power_swap = swap(power.at[0], power.at[1])
    send(power_swap)

    for t in range(tiles):
        at = cols(t)
        dres[:, at] = dot_nt(dlog[...], wide[2, at, :]).astype(BF16)
        if t == 0:
            moved_on((2, tiles - 1), 2, cols(tiles - 1))
        if t > 0 or tiles == 1:
            led_on((2, t), 2, at)
        product(1, hid_t, dres, at)
        scatter((1, t), 1, at)
        if t > 0:
            scatter_on((1, t - 1), 1, cols(t - 1))
    @pl.when(has_prev)
    def _():
        ups.wait_recv()

    @pl.when(has_next)
    def _():
        downs.wait_recv()

    def span_sums(m, carry):
        def body(r, carry):
            ahead, behind = differences(m, pl.ds(pl.multiple_of(r * step, step), step))
            return (
                carry[0] + fold(ahead * ahead),
                carry[1] + fold(behind * behind),
                carry[2] + fold(ahead * behind),
            )

        return lax.fori_loop(0, block // step, body, carry)

    carry = (zero, zero, zero)
    for m in range(3):
        carry = span_sums(m, carry)
    for k in range(3):
        sums[me, k] = carry[k]
    sums_sent, sums_landed = ticket(0), ticket(1)
    for d in range(1, n):
        remote(
            sums.at[me], sums.at[me], (ci, lax.rem(me + d, n)), sums_sent, sums_landed
        ).start()
    @pl.loop(0, tiles)
    def _(t):
        at = column(t)
        rows_t[at, :] = rows[:, at].T
    scatter_on((1, tiles - 1), 1, cols(tiles - 1))

    ends = [cols(t) for t in range(tiles - 1)]
    ends += [pl.ds(width - 2 * LANES, LANES), pl.ds(width - LANES, LANES)]
    for t, at in enumerate(ends):
        dlog[:, at] = (dot_nt(dres[...], wide[1, at, :]) * slope[:, at]).astype(BF16)
        product(0, rows_t, dlog, at)
        scatter((0, t), 0, at)
        if t > 0:
            moved_on((0, t - 1), 0, ends[t - 1])
        if t < tiles:

            @pl.when(moves)
            def _():
                scatter_home((2, t), 2, cols(t))
    moved_on((0, tiles), 0, ends[tiles])

    @pl.when(leads)
    def _():
        for t in range(tiles):
            scatter_home((2, t), 2, cols(t))

    def finish(key, m, cs, carry):
        arrive(to_home[key])

        def body(r, carry):
            at = pl.ds(pl.multiple_of(r * step, step), step)
            total = last[m, at, cs].astype(F32) * factor[m]
            edge[m, at, cs] = total
            return carry[0] + fold(total * tau[m][at, cs]), carry[1] + fold(total * total)

        return lax.fori_loop(0, block // step, body, carry)

    carry = (zero, zero)
    for t in range(tiles):
        scatter_home((1, t), 1, cols(t))
        if t == tiles - 1:
            for k, at in enumerate(ends):
                led_on((0, k), 0, at)
    landed(sums.at[pl.ds(0, n - 1)], sums_landed)

    def over_dp(ref, k):
        total = ref[0, k]
        for j in range(1, n):
            total = total + ref[j, k]
        return whole(total)

    sq_ahead, sq_behind, mixed = (over_dp(sums, k) for k in range(3))
    len_ahead = jnp.sqrt(sq_ahead + EPS)
    len_behind = jnp.sqrt(sq_behind + EPS)
    raw_sq = (
        sq_ahead / (len_ahead * len_ahead)
        + sq_behind / (len_behind * len_behind)
        + 2.0 * mixed / (len_ahead * len_behind)
    )
    raw_len = jnp.sqrt(raw_sq + EPS)
    spans[ci, 0] = jnp.broadcast_to(len_behind, (8, LANES))
    spans[ci, 1] = jnp.broadcast_to(len_ahead, (8, LANES))
    spans_sent, spans_landed = ticket(0), ticket(1)
    for d in range(1, c):
        remote(
            spans.at[ci], spans.at[ci], (lax.rem(ci + d, c), me), spans_sent, spans_landed
        ).start()
    by_ahead = 1.0 / (len_ahead * raw_len)
    by_behind = 1.0 / (len_behind * raw_len)
    for m in range(3):

        def body(r, _, m=m):
            at = pl.ds(pl.multiple_of(r * step, step), step)
            ahead, behind = differences(m, at)
            tau[m][at, :] = ahead * by_ahead + behind * by_behind
            return 0

        lax.fori_loop(0, block // step, body, 0)

    def flipped(source, cs, store):
        for low in range(0, block, LANES):
            at = pl.ds(low, min(LANES, block - low))
            for k in range(cs.start // LANES, (cs.start + cs.size) // LANES):
                top = min(classes - k * LANES, LANES)
                store(k * LANES, top, at, source[at, k * LANES : (k + 1) * LANES].T)

    def keep_tau(low, top, at, value):
        o_out[0, low : low + top, at] = value[0:top, :]

    def keep_grad(low, top, at, value):
        thin[1, low : low + top, at] = value[0:top, :]

    flipped(tau_out, everything, keep_tau)
    for i in range(tiles):
        carry = finish((2, i), 2, cols(i), carry)
        flipped(edge.at[2], cols(i), keep_grad)
        scatter_home((0, i), 0, ends[i])
    for t in range(tiles):
        carry = finish((1, t), 1, cols(t), carry)
    scatter_home((0, tiles), 0, ends[tiles])
    for t, at in enumerate(ends):
        carry = finish((0, t), 0, at, carry)
    arrive(power_swap)
    terms = (carry[0], carry[1], jnp.where(leads, power[0], power[1]))
    for k, term in enumerate(terms):
        late[me, k : k + 1, :] = jnp.sum(term, axis=0, keepdims=True)
    late[me, 3:8, :] = jnp.zeros((5, LANES), F32)
    late_sent, late_landed = ticket(0), ticket(1)
    for d in range(1, n):
        remote(
            late.at[me], late.at[me], (ci, lax.rem(me + d, n)), late_sent, late_landed
        ).start()
    landed(spans.at[pl.ds(0, c - 1)], spans_landed)
    arc = jnp.zeros((1, 1), F32)
    band = jnp.zeros((1, 1), F32)
    for k in range(c):
        length = spans[k, 0, 0:1, 0:1]
        arc = arc + jnp.where(k <= ci, length, 0.0)
        band = band + length
    band = band + spans[c - 1, 1, 0:1, 0:1]
    landed(late.at[pl.ds(0, n - 1)], late_landed)
    closing = late[0]
    for j in range(1, n):
        closing = closing + late[j]
    closing = jnp.sum(closing, axis=1, keepdims=True)
    along, g_g, energy_all = closing[0:1], closing[1:2], closing[2:3]

    goal = (ci + 1).astype(F32) / (c + 1) * band
    coef = jnp.where(jnp.full((1, 1), climb[0]) == 1, 2.0 * along, along + SPRING * (goal - arc) / band)
    tau_sq = raw_sq / (raw_sq + EPS)
    force_sq = g_g - 2.0 * coef * along + coef * coef * tau_sq
    scale = band / (c + 1) / jnp.sqrt(force_sq + EPS)
    push = scale * coef
    def small(value):
        return jnp.broadcast_to(value, (1, LANES))

    o_small[0:1, :] = small(energy_all)
    o_small[1:2, :] = small(arc / band)
    o_small[2:3, :] = small(0.5 * raw_len)
    for low in range(0, classes, LANES):
        at = pl.ds(low, min(LANES, classes - low))
        o_out[0, at, :] = thin[0, at, :] + (push * o_out[0, at, :] - scale * thin[1, at, :])

    for m in range(2):

        @pl.loop(0, block // step)
        def _(r):
            at = pl.ds(pl.multiple_of(r * step, step), step)
            tau[m][at, :] = own[m, at, :] + (push * tau[m][at, :] - scale * edge[m, at, :])
    @pl.when(has_next)
    def _():
        ups.wait_send()

    @pl.when(has_prev)
    def _():
        downs.wait_send()

    @pl.when(moves)
    def _():
        sent(stage, hop_out)
        sent(rows_out.at[:, 0:direct], row_sent)
        sent(others, pool_sent)
        sent(last, home_sent)
        for copy in (pool_swap, lab_swap, power_swap):
            copy.wait_send()

    for out in across_out + over_out:
        sent(stage, out)
    sent(from_core, core_sent)
    for out in pair_sent:
        sent(last, out)
    sent(sums.at[pl.ds(0, n - 1)], sums_sent)
    sent(spans.at[pl.ds(0, c - 1)], spans_sent)
    sent(late.at[pl.ds(0, n - 1)], late_sent)


def on_device(
    n,
    c,
    images_in,
    images_mid,
    images_out,
    ends_in,
    ends_mid,
    ends_out,
    data_pool,
    batch_rows,
    labels,
    climbing,
):
    block, width = images_in.shape[1], images_in.shape[2]
    classes = images_out.shape[2]
    depth = n * block
    batch = batch_rows.shape[1]
    pairs = n // 2
    sends, receives = semaphores(n, width // TILE, 3)
    vmem = pl.BlockSpec(memory_space=pltpu.VMEM)
    anywhere = pl.BlockSpec(memory_space=pl.ANY)
    scalar = pl.BlockSpec(memory_space=pltpu.SMEM)
    outs = pl.pallas_call(
        functools.partial(kernel, n, c, classes),
        out_shape=(
            pltpu.VMEM(images_in.shape, F32),
            pltpu.VMEM(images_mid.shape, F32),
            pltpu.VMEM((1, classes, block), F32),
            pltpu.VMEM((8, LANES), F32),
        ),
        in_specs=[anywhere] * 9 + [scalar],
        out_specs=[vmem] * 4,
        scratch_shapes=[
            pltpu.VMEM((3, block, width), F32),
            pltpu.VMEM((3, block, width), F32),
            pltpu.VMEM((2, width, block), F32),
            pltpu.VMEM((block, width), F32),
            pltpu.VMEM((3, depth, width), BF16),
            pltpu.VMEM((3, block, width), BF16),
            pltpu.VMEM((3, block, width), BF16),
            pltpu.VMEM((3, block, width), BF16),
            pltpu.VMEM((3, block, width), BF16),
            pltpu.VMEM(data_pool.shape, BF16),
            pltpu.VMEM((data_pool.shape[0], width // 2), BF16),
            pltpu.VMEM((2, 8, batch), jnp.int32),
            pltpu.VMEM((batch, LANES), jnp.int32),
            pltpu.VMEM((2, 8, batch), jnp.int32),
            pltpu.VMEM((2, 8, batch), jnp.int32),
            pltpu.VMEM((batch, depth), BF16),
            pltpu.VMEM((batch, depth), BF16),
            pltpu.VMEM((batch, width), F32),
            pltpu.VMEM((batch, width), BF16),
            pltpu.VMEM((batch, depth), BF16),
            pltpu.VMEM((depth, batch), BF16),
            pltpu.VMEM((width, batch), BF16),
            pltpu.VMEM((depth, batch), BF16),
            pltpu.VMEM((batch, width), BF16),
            pltpu.VMEM((batch, depth), BF16),
            pltpu.VMEM((3, depth, width), BF16),
            pltpu.VMEM((3, pairs, block, width), BF16),
            pltpu.VMEM((3, max(pairs - 1, 1), block, width), BF16),
            pltpu.VMEM((3, block, width), BF16),
            pltpu.VMEM((2, 8, LANES), F32),
            pltpu.VMEM((n, 3, 8, LANES), F32),
            pltpu.VMEM((c, 2, 8, LANES), F32),
            pltpu.VMEM((n, 8, LANES), F32),
            pltpu.SemaphoreType.DMA((8 + c // 2,)),
            pltpu.SemaphoreType.DMA((sends,)),
            pltpu.SemaphoreType.DMA((receives,)),
        ],
        compiler_params=pltpu.CompilerParams(
            collective_id=0, has_side_effects=True, vmem_limit_bytes=60 * 1024 * 1024
        ),
    )(
        images_in,
        images_mid,
        jnp.swapaxes(images_out, 1, 2),
        ends_in,
        ends_mid,
        jnp.swapaxes(ends_out, 1, 2),
        data_pool,
        batch_rows,
        labels,
        climbing,
    )
    return (outs[0], outs[1], jnp.swapaxes(outs[2], 1, 2), *(outs[3][k, 0:1] for k in range(3)))


def solution(mesh):
    placed = (
        P("chain", "dp", None),
        P("chain", "dp", None),
        P("chain", "dp", None),
        P(None, "dp", None),
        P(None, "dp", None),
        P(None, "dp", None),
        P("dp", None),
        P("chain", "dp"),
        P("chain", "dp"),
        P("chain"),
    )
    return jax.shard_map(
        functools.partial(on_device, mesh.shape["dp"], mesh.shape["chain"]),
        mesh=mesh,
        in_specs=placed,
        out_specs=(
            P("chain", "dp", None),
            P("chain", "dp", None),
            P("chain", "dp", None),
            P("chain"),
            P("chain"),
            P("chain"),
        ),
        check_vma=False,
    )
```
